32 devices in a mesh: batch: 4 (over x, core), rows: 8 (over z, y).
Axes of the slice: x: 2, y: 2, z: 4, core: 2. Of those that a mesh axis runs over, the one named last changes fastest.
Arguments:
- feat_quarter: bfloat16 [4, 128, 512, 256], P('batch', 'rows'), may hold values from -12 to 12
- feat_eighth: bfloat16 [4, 64, 256, 256], P('batch', 'rows'), may hold values from -12 to 12
- feat_sixteenth: bfloat16 [4, 32, 128, 256], P('batch', 'rows'), may hold values from -12 to 12
- feat_thirty: bfloat16 [4, 16, 64, 256], P('batch', 'rows'), may hold values from -12 to 12
- labels: int32 [4, 128, 512], P('batch', 'rows'), may hold values from 0 to 255, as said below
- first_weights: bfloat16 [4, 3, 3, 256, 128], replicated, may hold values from -0.125 to 0.125
- inner_weights: bfloat16 [3, 3, 3, 128, 128], replicated, may hold values from -0.1875 to 0.1875
- norm_gain: float32 [7, 128], replicated, may hold values from 0.1 to 1.9
- norm_shift: float32 [7, 128], replicated, may hold values from -3 to 3
- class_weight: bfloat16 [128, 19], replicated, may hold values from -0.5 to 0.5
- class_bias: float32 [19], replicated, may hold values from -3 to 3
Outputs:
- logits: bfloat16 [4, 19, 128, 512], P('batch', None, 'rows')
- mean_loss: float32 [], replicated
The draws below stay inside these ranges and needn't reach their ends.
Inputs may be any that keep to these rules, and one draw needn't show every extreme that they name: `labels`: values 0 to 18 name classes; 255 marks a pixel without a label.
All inputs are finite; a program needn't handle non-finite values.
Results may differ from the reference program's by a relative error of at most 0.008.
Values may be sent and summed in bfloat16 or wider, within the bound.
A program may use at most 128 MiB of HBM per device.

```python
import jax
import jax.numpy as jnp
from jax import lax

C_IN = 256
HEAD = 128
CLASSES = 19
GROUPS = 32
COLS4 = 512
IMAGES = 4
QUARTER_ROWS = 128


def feature_map(key, row_count, col_count, marker):
    level_key = jax.random.fold_in(key, marker)
    base_key, offset_key, slope_key = jax.random.split(level_key, 3)
    array_shape = (IMAGES, row_count, col_count, C_IN)
    row_ramp = ((jnp.arange(row_count, dtype=jnp.float32) + 0.5) / row_count)[None, :, None, None]
    base = jax.random.normal(base_key, array_shape, jnp.float32)
    slope_rate = jax.random.uniform(slope_key, (IMAGES, 1, 1, 1), jnp.float32, 1.0, 1.6)
    offset = jax.random.normal(offset_key, (IMAGES, 1, 1, C_IN), jnp.float32) * 0.5
    row_scale = jnp.exp(1.4 * slope_rate * (row_ramp - 0.5))
    values = base * row_scale + 2.0 * offset * row_ramp
    return jnp.clip(values, -12.0, 12.0).astype(jnp.bfloat16)


def draw_feat_quarter(key, part):
    return feature_map(key, QUARTER_ROWS, COLS4, 11)


def draw_feat_eighth(key, part):
    return feature_map(key, QUARTER_ROWS // 2, COLS4 // 2, 12)


def draw_feat_sixteenth(key, part):
    return feature_map(key, QUARTER_ROWS // 4, COLS4 // 4, 13)


def draw_feat_thirty(key, part):
    return feature_map(key, QUARTER_ROWS // 8, COLS4 // 8, 14)


def draw_labels(key, part):
    class_key, drop_key, major_key, choose_key = jax.random.split(jax.random.fold_in(key, 7), 4)
    array_shape = (IMAGES, QUARTER_ROWS, COLS4)
    classes = jax.random.randint(class_key, array_shape, 0, CLASSES)
    majors = jax.random.randint(major_key, (IMAGES, QUARTER_ROWS // 8), 0, CLASSES)
    row_index = jnp.arange(QUARTER_ROWS, dtype=jnp.int32)
    block_major = majors[:, row_index // 8][:, :, None]
    choose = jax.random.randint(choose_key, array_shape, 0, 1000)
    classes = jnp.where(choose < 700, block_major, classes)
    chance = jax.random.randint(drop_key, array_shape, 0, 1000)
    drop_limit = 40 + 700 * row_index * row_index // (QUARTER_ROWS * QUARTER_ROWS)
    return jnp.where(chance < drop_limit[None, :, None], 255, classes).astype(jnp.int32)


def centred(key, dims, scale, bound, held_as=jnp.bfloat16):
    drawn = jax.random.normal(key, dims, jnp.float32) * scale
    return jnp.minimum(jnp.maximum(drawn, -bound), bound).astype(held_as)


def setup_inputs(seed: int = 0) -> dict:
    arg_keys = jax.random.split(jax.random.key(seed), 12)
    feat_quarter = draw_feat_quarter(jax.random.fold_in(arg_keys[11], 71), 0)
    feat_eighth = draw_feat_eighth(jax.random.fold_in(arg_keys[11], 71), 0)
    feat_sixteenth = draw_feat_sixteenth(jax.random.fold_in(arg_keys[11], 71), 0)
    feat_thirty = draw_feat_thirty(jax.random.fold_in(arg_keys[11], 71), 0)
    labels = draw_labels(jax.random.fold_in(arg_keys[11], 71), 0)
    first_weights = centred(arg_keys[5], (4, 3, 3, C_IN, HEAD), (9 * C_IN) ** -0.5, 0.125)
    inner_weights = centred(arg_keys[6], (3, 3, 3, HEAD, HEAD), (9 * HEAD) ** -0.5, 0.1875)
    norm_gain = jnp.clip(1.0 + 0.18 * jax.random.normal(arg_keys[7], (7, HEAD), jnp.float32), 0.1, 1.9)
    norm_shift = centred(arg_keys[8], (7, HEAD), 0.5, 3.0, jnp.float32)
    class_weight = centred(arg_keys[9], (HEAD, CLASSES), HEAD ** -0.5, 0.5)
    class_bias = centred(arg_keys[10], (CLASSES,), 0.5, 3.0, jnp.float32)
    return {"feat_quarter": feat_quarter, "feat_eighth": feat_eighth, "feat_sixteenth": feat_sixteenth, "feat_thirty": feat_thirty, "labels": labels, "first_weights": first_weights, "inner_weights": inner_weights, "norm_gain": norm_gain, "norm_shift": norm_shift, "class_weight": class_weight, "class_bias": class_bias}


NORM_FLOOR = 0.05

def conv_rows(framed, weight):
    row_count = framed.shape[0] - 2
    col_count = framed.shape[1]
    padded = jnp.pad(framed, ((0, 0), (1, 1), (0, 0)))
    result = jnp.zeros((row_count, col_count, weight.shape[3]), jnp.float32)
    for downward in range(3):
        for across in range(3):
            window = padded[downward:downward + row_count, across:across + col_count, :]
            result = result + jnp.einsum('rwc,cd->rwd', window.astype(jnp.float32), weight[downward, across].astype(jnp.float32))
    return result

def heighten(padded):
    row_count = padded.shape[0] - 2
    middle = padded[1:-1]
    even_rows = 0.75 * middle + 0.25 * padded[:-2]
    odd_rows = 0.75 * middle + 0.25 * padded[2:]
    inner_rows = jnp.stack([even_rows, odd_rows], axis=1).reshape(2 * row_count, padded.shape[1], padded.shape[2])
    upper_row = 0.75 * padded[0] + 0.25 * padded[1]
    lower_row = 0.75 * padded[-1] + 0.25 * padded[-2]
    return jnp.concatenate([upper_row[None], inner_rows, lower_row[None]], axis=0)

def widen(field):
    left_side = jnp.concatenate([field[:, :1], field[:, :-1]], axis=1)
    right_side = jnp.concatenate([field[:, 1:], field[:, -1:]], axis=1)
    even_cols = 0.75 * field + 0.25 * left_side
    odd_cols = 0.75 * field + 0.25 * right_side
    return jnp.stack([even_cols, odd_cols], axis=2).reshape(field.shape[0], 2 * field.shape[1], field.shape[2])

def group_sum(values):
    channel_sums = lax.optimization_barrier(jnp.sum(values, axis=(0, 1)))
    return channel_sums.reshape(GROUPS, -1).sum(axis=1)

def spread(values, width):
    return jnp.repeat(values, width // GROUPS)

def finish(values, group_mean, group_var, gain, shift):
    width = values.shape[2]
    factor = gain * lax.rsqrt(spread(group_var, width) + NORM_FLOOR)
    return jnp.maximum((values - spread(group_mean, width)) * factor + shift, 0.0).astype(jnp.bfloat16)

def normalize(values, gain, shift):
    pixels = values.shape[0] * values.shape[1] * (values.shape[2] // GROUPS)
    group_mean = group_sum(values) / pixels
    centered = values - spread(group_mean, values.shape[2])
    group_var = group_sum(centered * centered) / pixels
    return finish(values, group_mean, group_var, gain, shift)

def upsample(active):
    padded = jnp.pad(active, ((1, 1), (0, 0), (0, 0)), mode='edge').astype(jnp.float32)
    return widen(heighten(padded)[1:-1]).astype(jnp.bfloat16)

def reference(feat_quarter, feat_eighth, feat_sixteenth, feat_thirty, labels, first_weights, inner_weights, norm_gain, norm_shift, class_weight, class_bias):

    def section(image_in, weight, layer_index):
        framed = jnp.pad(image_in, ((1, 1), (0, 0), (0, 0)))
        return normalize(conv_rows(framed, weight), norm_gain[layer_index], norm_shift[layer_index])

    def one_image(image_items):
        quarter_in, eighth_in, sixteenth_in, thirty_in, label_map = image_items
        quarter = section(quarter_in, first_weights[0], 0)
        eighth = upsample(section(eighth_in, first_weights[1], 1))
        sixteenth = upsample(section(upsample(section(sixteenth_in, first_weights[2], 2)), inner_weights[0], 4))
        coarse = upsample(section(thirty_in, first_weights[3], 3))
        thirty = upsample(section(upsample(section(coarse, inner_weights[1], 5)), inner_weights[2], 6))
        combined = (quarter.astype(jnp.float32) + eighth.astype(jnp.float32) + sixteenth.astype(jnp.float32) + thirty.astype(jnp.float32)).astype(jnp.bfloat16)
        scores = jnp.einsum('rwc,ck->krw', combined.astype(jnp.float32), class_weight.astype(jnp.float32)) + class_bias.astype(jnp.float32)[:, None, None]
        log_total = jnp.log(lax.optimization_barrier(jnp.sum(jnp.exp(scores), axis=0)))
        classes = jnp.arange(scores.shape[0], dtype=jnp.int32)[:, None, None]
        picked = lax.optimization_barrier(jnp.sum(jnp.where(classes == label_map[None], scores, 0.0), axis=0))
        usable = label_map != 255
        loss_total = jnp.sum(jnp.where(usable, log_total - picked, 0.0))
        valid_count = jnp.sum(usable.astype(jnp.float32))
        return (scores.astype(jnp.bfloat16), loss_total, valid_count)
    logits, totals, counts = lax.map(one_image, (feat_quarter, feat_eighth, feat_sixteenth, feat_thirty, labels))
    mean_loss = jnp.sum(totals) / jnp.maximum(jnp.sum(counts), 1.0)
    return (logits, mean_loss)
```

```python
import functools

import jax
import jax.numpy as jnp
from jax import lax
from jax.experimental import pallas as pl
from jax.experimental.pallas import tpu as pltpu
from jax.sharding import PartitionSpec as P

GROUPS = 32
NORM_FLOOR = 0.05
IGNORED = 255
Q_CHUNKS = 8
E_CHUNKS = 2
MESH = pl.DeviceIdType.MESH
F32 = jnp.float32
BF16 = jnp.bfloat16


def group_fold(x):
    width = x.shape[-1]
    lane = lax.broadcasted_iota(jnp.int32, x.shape, x.ndim - 1)
    step = 1
    while step < width // GROUPS:
        ahead = pltpu.roll(x, width - step, x.ndim - 1)
        behind = pltpu.roll(x, step, x.ndim - 1)
        x = x + jnp.where(lax.rem(lane, 2 * step) < step, ahead, behind)
        step *= 2
    return x


def doubling(rows, cols, source_axis):
    source = lax.broadcasted_iota(jnp.int32, (rows, cols), source_axis)
    target = lax.broadcasted_iota(jnp.int32, (rows, cols), 1 - source_axis)
    count = (rows, cols)[source_axis]
    near = lax.div(target, 2)
    far = jnp.clip(near + 2 * lax.rem(target, 2) - 1, 0, count - 1)
    return (
        0.75 * (source == near).astype(F32) + 0.25 * (source == far).astype(F32)
    ).astype(BF16)


def conv_block(x_ref, flat_ref, start, rows):
    cols, depth = x_ref.shape[1:]
    width = flat_ref.shape[1] // 3
    lhs = jnp.concatenate(
        [
            x_ref[pl.ds(start + down, rows)].reshape(rows * cols, depth)
            for down in range(3)
        ],
        axis=1,
    )
    taps = jnp.dot(lhs, flat_ref[...], preferred_element_type=F32)
    col = lax.rem(lax.broadcasted_iota(jnp.int32, (rows * cols, width), 0), cols)
    left = jnp.where(col == 0, 0.0, pltpu.roll(taps[:, :width], 1, 0))
    right = jnp.where(col == cols - 1, 0.0, pltpu.roll(taps[:, 2 * width :], rows * cols - 1, 0))
    return (taps[:, width : 2 * width] + left + right).reshape(rows, cols, width)


def conv_to(x_ref, flat_ref, y_ref, stat_ref, start, rows, offset):
    y = conv_block(x_ref, flat_ref, start, rows)
    cols = y.shape[1]
    y_ref[pl.ds(start + offset, rows)] = y
    sums = jnp.sum(y, axis=1, keepdims=True)
    centred = y - sums / cols
    stat_ref[pl.ds(start, rows), 0:1] = sums
    stat_ref[pl.ds(start, rows), 1:2] = jnp.sum(centred * centred, axis=1, keepdims=True)


def head_kernel(
    shape,
    q, e, s, t, labels, first_w, inner_w, gain, shift, class_w, bias,
    out, loss_out,
    q_in, e_in, s_in, t_in, w_q, w_e, w_s, w_t, w_i,
    q_y, e_y, s_y, t_y, s_grown, s_y2, t_grown, t_y2, t_grown2, t_y3,
    q_stat, e_stat, s_stat, t_stat, s_stat2, t_stat2, t_stat3,
    slab, slabs, class_f, class_pad, up_t, up_s, coarse, wide, scores_q, loss_slab, loss_slabs,
    local_sem, edge_send, edge_recv, slab_send, slab_recv, loss_send, loss_recv,
):
    size, images = shape["rows"], shape["batch"]
    total = size * images
    me, image = lax.axis_index("rows"), lax.axis_index("batch")
    flat = image * size + me
    width = q_y.shape[2]
    classes = class_w.shape[0]

    def device_at(distance):
        number = lax.rem(flat + distance, total)
        return {"batch": lax.div(number, size), "rows": lax.rem(number, size)}

    barrier = pltpu.get_barrier_semaphore()

    def greet(distance, carry):
        pl.semaphore_signal(
            barrier, inc=1, device_id=device_at(distance), device_id_type=MESH
        )
        return carry

    lax.fori_loop(1, total, greet, 0)

    fetched = []

    def fetch(source, target):
        copy = pltpu.make_async_copy(source, target, local_sem.at[len(fetched)])
        copy.start()
        fetched.append(copy)
        return copy

    def fetch_weights(source, target):
        depth = source.shape[2]
        return [
            fetch(
                source.at[down, across],
                target.at[down * depth : (down + 1) * depth, across * width : (across + 1) * width],
            )
            for down in range(3)
            for across in range(3)
        ]

    def settle(copies):
        for copy in copies:
            copy.wait()

    q_rows, q_cols = q.shape[:2]
    e_rows, s_rows, t_rows = e.shape[0], s.shape[0], t.shape[0]
    got_q = fetch_weights(first_w.at[0], w_q) + [fetch(q, q_in.at[1 : q_rows + 1])]
    got_t = fetch_weights(first_w.at[3], w_t) + [fetch(t, t_in.at[1 : t_rows + 1])]
    got_s = fetch_weights(first_w.at[2], w_s) + [fetch(s, s_in.at[1 : s_rows + 1])]
    got_i = [c for i in range(3) for c in fetch_weights(inner_w.at[i], w_i.at[i])]
    got_e = fetch_weights(first_w.at[1], w_e) + [fetch(e, e_in.at[1 : e_rows + 1])]

    def exists(offset):
        return me + offset < size if offset > 0 else me + offset >= 0

    def neighbour(offset):
        return {"rows": lax.rem(me + offset + size, size)}

    sent = []

    def edge(source_of, target_of, number, offset):
        own = source_of.shape[0]
        return pltpu.make_async_remote_copy(
            src_ref=source_of,
            dst_ref=target_of,
            send_sem=edge_send.at[number],
            recv_sem=edge_recv.at[number],
            device_id=neighbour(offset),
            device_id_type=MESH,
        )

    def edges(source, first, last, target, before, after, number, part=None):
        def at(ref, row):
            return ref.at[row] if part is None else ref.at[row, part]

        return [
            (edge(at(source, last), at(target, before), number, 1), 1),
            (edge(at(source, first), at(target, after), number + 1, -1), -1),
        ]

    def send(pairs):
        for copy, offset in pairs:
            pl.when(exists(offset))(copy.start)

    def arrive(pairs):
        for copy, offset in pairs:
            pl.when(exists(-offset))(copy.wait_recv)

    def leave(pairs):
        for copy, offset in pairs:
            pl.when(exists(offset))(copy.wait_send)

    def feature_edges(source, target, number, part=None):
        count = source.shape[0]
        return edges(source, 0, count - 1, target, 0, count + 1, number, part)

    def band_edges(field, number):
        count = field.shape[0] - 2
        return edges(field, 1, count, field, 0, count + 1, number)

    t_edges, s_edges = feature_edges(t, t_in, 0), feature_edges(s, s_in, 2)
    t_y_edges, s_y_edges, t_y2_edges = band_edges(t_y, 4), band_edges(s_y, 6), band_edges(t_y2, 8)
    coarse_edges = band_edges(coarse, 10)

    def e_edges(chunk):
        part = pl.ds(pl.multiple_of(chunk * (e.shape[1] // E_CHUNKS), 16), e.shape[1] // E_CHUNKS)
        return feature_edges(e, e_in, 12 + 2 * chunk, part)

    def q_edges(chunk):
        part = pl.ds(pl.multiple_of(chunk * (q_cols // Q_CHUNKS), 16), q_cols // Q_CHUNKS)
        return feature_edges(q, q_in, 12 + 2 * E_CHUNKS + 2 * chunk, part)

    def each_chunk(count, act):
        def step(chunk, carry):
            act(chunk)
            return carry

        lax.fori_loop(0, count, step, 0)

    @pl.when(me == 0)
    def _():
        for field in (q_in, e_in, s_in, t_in):
            field[0] = jnp.zeros(field.shape[1:], BF16)

    @pl.when(me == size - 1)
    def _():
        for field in (q_in, e_in, s_in, t_in):
            field[field.shape[0] - 1] = jnp.zeros(field.shape[1:], BF16)

    slab[...] = jnp.zeros(slab.shape, F32)
    loss_slab[...] = jnp.zeros(loss_slab.shape, F32)
    up_t[...] = doubling(*up_t.shape, 1)
    up_s[...] = doubling(*up_s.shape, 1)
    class_f[...] = jnp.zeros(class_f.shape, F32)
    class_f[0:classes] = class_w[...].astype(F32)
    class_pad[...] = class_f[...].astype(BF16)
    padded = class_f.shape[0]
    spot = lax.broadcasted_iota(jnp.int32, (padded, classes), 0)
    lane = lax.broadcasted_iota(jnp.int32, (padded, classes), 1)
    bias_col = jnp.sum(jnp.where(spot == lane, bias[...], 0.0), axis=1, keepdims=True)

    pl.semaphore_wait(barrier, total - 1)
    send(t_edges)
    send(s_edges)

    def slab_copy(number, distance):
        return pltpu.make_async_remote_copy(
            src_ref=slab.at[number],
            dst_ref=slabs.at[number, me],
            send_sem=slab_send.at[number, distance],
            recv_sem=slab_recv.at[number, distance],
            device_id=neighbour(distance),
            device_id_type=MESH,
        )

    def slab_arrival(number, distance):
        sender = lax.rem(me - distance + size, size)
        return pltpu.make_async_remote_copy(
            src_ref=slab.at[number],
            dst_ref=slabs.at[number, sender],
            send_sem=slab_send.at[number, distance],
            recv_sem=slab_recv.at[number, distance],
            device_id=neighbour(distance),
            device_id_type=MESH,
        )

    def announce(number, fields):
        for place, (stat, cols) in enumerate(fields):
            rows = stat.shape[0]
            sums = stat[:, 0:1]
            channel = jnp.sum(sums, axis=0)
            mean = group_fold(channel) / (rows * cols * (width // GROUPS))
            strays = sums / cols - mean
            squares = jnp.sum(stat[:, 1:2] + cols * (strays * strays), axis=0)
            slab[number, 2 * place : 2 * place + 1] = channel
            slab[number, 2 * place + 1 : 2 * place + 2] = squares
        for distance in range(1, size):
            slab_copy(number, distance).start()
        slabs[number, me] = slab[number]

    def gather(number, counts):
        for distance in range(1, size):
            slab_arrival(number, distance).wait_recv()
        every = slabs[number]
        every = group_fold(every.reshape(size * every.shape[1], width)).reshape(every.shape)
        result = []
        for place, count in enumerate(counts):
            means = every[:, 2 * place : 2 * place + 1] / count
            mean = jnp.sum(means, axis=0) / size
            strays = means - mean
            squares = jnp.sum(
                every[:, 2 * place + 1 : 2 * place + 2] + count * (strays * strays), axis=0
            )
            result.append((mean, squares / (count * size)))
        return result

    def count_of(rows, cols):
        return rows * cols * (width // GROUPS)

    def activation(stat, layer):
        mean, var = stat
        factor = gain[layer : layer + 1] * lax.rsqrt(var + NORM_FLOOR)
        offset = shift[layer : layer + 1]
        return lambda y: jnp.maximum((y - mean) * factor + offset, 0.0).astype(BF16)

    def grow(field, grown, up, act):
        own = field.shape[0] - 2

        @pl.when(me == 0)
        def _():
            field[0] = field[1]

        @pl.when(me == size - 1)
        def _():
            field[own + 1] = field[own]

        lines = jnp.concatenate([act(field[row]) for row in range(own + 2)], axis=1)
        lines = jnp.dot(up[...], lines, preferred_element_type=F32)
        for row in range(own + 1):
            here = lines[:, row * width : (row + 1) * width]
            below = lines[:, (row + 1) * width : (row + 2) * width]
            grown[2 * row] = (0.75 * here + 0.25 * below).astype(BF16)
            grown[2 * row + 1] = (0.25 * here + 0.75 * below).astype(BF16)

        @pl.when(me == 0)
        def _():
            grown[0] = jnp.zeros(grown.shape[1:], BF16)

        @pl.when(me == size - 1)
        def _():
            grown[2 * own + 1] = jnp.zeros(grown.shape[1:], BF16)

    def convolve(x_ref, flat_ref, y_ref, stat_ref, rows, offset):
        count = x_ref.shape[0] - 2

        def step(index, carry):
            conv_to(x_ref, flat_ref, y_ref, stat_ref, index * rows, rows, offset)
            return carry

        lax.fori_loop(0, count // rows, step, 0)

    def rows_within(count, cols):
        return max(r for r in range(1, count + 1) if count % r == 0 and (r == 1 or r * cols <= 1024))

    def q_blocks(first, last, chunk):
        def step(index, carry):
            if chunk is not None:
                send(q_edges(chunk + index - first))
            conv_to(q_in, w_q, q_y, q_stat, 1 + 2 * index, 2, 0)
            return carry

        lax.fori_loop(first, last, step, 0)

    blocks = (q_rows - 2) // 2
    settle(got_q)
    q_blocks(0, 2, None)

    settle(got_t)
    arrive(t_edges)
    conv_to(t_in, w_t, t_y, t_stat, 0, t_rows, 1)
    settle(got_s)
    arrive(s_edges)
    conv_to(s_in, w_s, s_y, s_stat, 0, s_rows, 1)
    announce(0, [(t_stat, t.shape[1]), (s_stat, s.shape[1])])
    send(t_y_edges)
    send(s_y_edges)
    for chunk in range(E_CHUNKS):
        send(e_edges(chunk))
    q_blocks(2, 4, 0)

    t_norm, s_norm = gather(0, [count_of(t_rows, t.shape[1]), count_of(s_rows, s.shape[1])])
    settle(got_i)
    arrive(t_y_edges)
    grow(t_y, t_grown, up_t, activation(t_norm, 3))
    convolve(t_grown, w_i.at[1], t_y2, t_stat2, rows_within(2 * t_rows, 2 * t.shape[1]), 1)
    arrive(s_y_edges)
    grow(s_y, s_grown, up_s, activation(s_norm, 2))
    convolve(s_grown, w_i.at[0], s_y2, s_stat2, rows_within(2 * s_rows, 2 * s.shape[1]), 0)
    announce(1, [(t_stat2, 2 * t.shape[1]), (s_stat2, 2 * s.shape[1])])
    send(t_y2_edges)
    q_blocks(4, 6, 2)
    settle(got_e)
    for chunk in range(E_CHUNKS):
        arrive(e_edges(chunk))
    convolve(e_in, w_e, e_y, e_stat, rows_within(e_rows, e.shape[1]), 0)

    t_norm, s_norm = gather(
        1, [count_of(2 * t_rows, 2 * t.shape[1]), count_of(2 * s_rows, 2 * s.shape[1])]
    )
    each_chunk(Q_CHUNKS - 4, lambda chunk: send(q_edges(chunk + 4)))
    arrive(t_y2_edges)
    grow(t_y2, t_grown2, up_s, activation(t_norm, 5))
    convolve(t_grown2, w_i.at[2], t_y3, t_stat3, rows_within(4 * t_rows, 4 * t.shape[1]), 0)
    announce(2, [(t_stat3, 4 * t.shape[1]), (e_stat, e.shape[1])])
    q_blocks(6, blocks, None)
    each_chunk(Q_CHUNKS, lambda chunk: arrive(q_edges(chunk)))

    def border(index, carry):
        conv_to(q_in, w_q, q_y, q_stat, index * (q_rows - 1), 1, 0)
        return carry

    lax.fori_loop(0, 2, border, 0)
    announce(3, [(q_stat, q_cols)])

    t_norm, e_norm = gather(
        2, [count_of(4 * t_rows, 4 * t.shape[1]), count_of(e_rows, e.shape[1])]
    )
    e_act, s_act, t_act = activation(e_norm, 1), activation(s_norm, 4), activation(t_norm, 6)
    weight = class_pad[...]
    weights = jnp.concatenate([weight] * 3, axis=1)
    across = (((1,), (1,)), ((), ()))

    def project(row, carry):
        lines = jnp.concatenate([e_act(e_y[row]), s_act(s_y2[row]), t_act(t_y3[row])], axis=1)
        coarse[row + 1] = lax.dot_general(weights, lines, across, preferred_element_type=F32)
        return carry

    lax.fori_loop(0, e_rows, project, 0)
    send(coarse_edges)

    (q_norm,) = gather(3, [count_of(q_rows, q_cols)])
    q_act = activation(q_norm, 0)

    def score(row, carry):
        scores_q[row] = (
            lax.dot_general(weight, q_act(q_y[row]), across, preferred_element_type=F32) + bias_col
        )
        return carry

    lax.fori_loop(0, q_rows, score, 0)
    up_cols = doubling(e.shape[1], q_cols, 0)
    arrive(coarse_edges)

    @pl.when(me == 0)
    def _():
        coarse[0] = coarse[1]

    @pl.when(me == size - 1)
    def _():
        coarse[e_rows + 1] = coarse[e_rows]

    lines = coarse[...].reshape((e_rows + 2) * padded, e.shape[1])
    high = lines.astype(BF16)
    low = (lines - high.astype(F32)).astype(BF16)
    lines = jnp.dot(high, up_cols, preferred_element_type=F32) + jnp.dot(
        low, up_cols, preferred_element_type=F32
    )
    wide[...] = lines.reshape(wide.shape)
    kind = lax.broadcasted_iota(jnp.int32, (padded, q_cols), 0)

    def finish(row, grown):
        scores = scores_q[row] + grown
        out[row] = scores.astype(BF16)
        powers = jnp.where(kind < classes, jnp.exp(scores), 0.0)
        log_total = jnp.log(jnp.sum(powers, axis=0, keepdims=True))
        label = labels[pl.ds(row, 1), :]
        picked = jnp.sum(jnp.where(kind == label, scores, 0.0), axis=0, keepdims=True)
        usable = label != IGNORED
        return jnp.where(usable, log_total - picked, 0.0), usable.astype(F32)

    def pair(index, carry):
        here = wide[index + 1]
        upper = finish(2 * index, 0.25 * wide[index] + 0.75 * here)
        lower = finish(2 * index + 1, 0.75 * here + 0.25 * wide[index + 2])
        return carry[0] + upper[0] + lower[0], carry[1] + upper[1] + lower[1]

    zero = jnp.zeros((1, q_cols), F32)
    sums = lax.fori_loop(0, e_rows, pair, (zero, zero))
    for place, line in enumerate(sums):
        loss_slab[place : place + 1] = sum(
            line[:, k * width : (k + 1) * width] for k in range(q_cols // width)
        )

    def loss_copy(distance, sender):
        return pltpu.make_async_remote_copy(
            src_ref=loss_slab,
            dst_ref=loss_slabs.at[sender],
            send_sem=loss_send.at[distance],
            recv_sem=loss_recv.at[distance],
            device_id=device_at(distance),
            device_id_type=MESH,
        )

    def loss_go(distance, carry):
        loss_copy(distance, flat).start()
        return carry

    def loss_come(distance, carry):
        loss_copy(distance, lax.rem(flat - distance + total, total)).wait_recv()
        return carry

    def loss_gone(distance, carry):
        loss_copy(distance, flat).wait_send()
        return carry

    lax.fori_loop(1, total, loss_go, 0)
    loss_slabs[flat] = loss_slab[...]
    for pairs in (t_edges, s_edges, t_y_edges, s_y_edges, t_y2_edges, coarse_edges):
        leave(pairs)
    for chunk in range(E_CHUNKS):
        leave(e_edges(chunk))
    each_chunk(Q_CHUNKS, lambda chunk: leave(q_edges(chunk)))
    for number in range(4):
        for distance in range(1, size):
            slab_copy(number, distance).wait_send()
    lax.fori_loop(1, total, loss_come, 0)
    ends = jnp.sum(jnp.sum(loss_slabs[...], axis=0), axis=1, keepdims=True)
    loss_out[...] = jnp.broadcast_to(ends[0:1] / jnp.maximum(ends[1:2], 1.0), loss_out.shape)
    lax.fori_loop(1, total, loss_gone, 0)


def make_per_device(shape):
    def per_device(
        feat_quarter,
        feat_eighth,
        feat_sixteenth,
        feat_thirty,
        labels,
        first_weights,
        inner_weights,
        norm_gain,
        norm_shift,
        class_weight,
        class_bias,
    ):
        q, e, s, t = feat_quarter[0], feat_eighth[0], feat_sixteenth[0], feat_thirty[0]
        size = shape["rows"]
        total = size * shape["batch"]
        depth, width = first_weights.shape[3:]
        classes = class_weight.shape[1]
        padded = -(-classes // 8) * 8
        (q_rows, q_cols), (e_rows, e_cols) = q.shape[:2], e.shape[:2]
        (s_rows, s_cols), (t_rows, t_cols) = s.shape[:2], t.shape[:2]

        def framed(rows, cols, channels, kind=BF16):
            return pltpu.VMEM((rows + 2, cols, channels), kind)

        def field(rows, cols):
            return pltpu.VMEM((rows, cols, width), F32)

        def stat(rows):
            return pltpu.VMEM((rows, 8, width), F32)

        edges = 12 + 2 * E_CHUNKS + 2 * Q_CHUNKS
        scratch = [
            framed(q_rows, q_cols, depth),
            framed(e_rows, e_cols, depth),
            framed(s_rows, s_cols, depth),
            framed(t_rows, t_cols, depth),
            *[pltpu.VMEM((3 * depth, 3 * width), BF16)] * 4,
            pltpu.VMEM((3, 3 * width, 3 * width), BF16),
            field(q_rows, q_cols),
            field(e_rows, e_cols),
            framed(s_rows, s_cols, width, F32),
            framed(t_rows, t_cols, width, F32),
            framed(2 * s_rows, 2 * s_cols, width),
            field(2 * s_rows, 2 * s_cols),
            framed(2 * t_rows, 2 * t_cols, width),
            framed(2 * t_rows, 2 * t_cols, width, F32),
            framed(4 * t_rows, 4 * t_cols, width),
            field(4 * t_rows, 4 * t_cols),
            stat(q_rows),
            stat(e_rows),
            stat(s_rows),
            stat(t_rows),
            stat(2 * s_rows),
            stat(2 * t_rows),
            stat(4 * t_rows),
            pltpu.VMEM((4, 8, width), F32),
            pltpu.VMEM((4, size, 8, width), F32),
            pltpu.VMEM((padded, width), F32),
            pltpu.VMEM((padded, width), BF16),
            pltpu.VMEM((2 * t_cols, t_cols), BF16),
            pltpu.VMEM((2 * s_cols, s_cols), BF16),
            framed(e_rows, padded, e_cols, F32),
            framed(e_rows, padded, q_cols, F32),
            pltpu.VMEM((q_rows, padded, q_cols), F32),
            pltpu.VMEM((8, width), F32),
            pltpu.VMEM((total, 8, width), F32),
            pltpu.SemaphoreType.DMA((80,)),
            pltpu.SemaphoreType.DMA((edges,)),
            pltpu.SemaphoreType.DMA((edges,)),
            pltpu.SemaphoreType.DMA((4, size)),
            pltpu.SemaphoreType.DMA((4, size)),
            pltpu.SemaphoreType.DMA((total,)),
            pltpu.SemaphoreType.DMA((total,)),
        ]
        held = pl.BlockSpec(memory_space=pltpu.VMEM)
        away = pl.BlockSpec(memory_space=pl.ANY)
        scores, loss = pl.pallas_call(
            functools.partial(head_kernel, shape),
            out_shape=(
                jax.ShapeDtypeStruct((q_rows, padded, q_cols), BF16),
                jax.ShapeDtypeStruct((8, width), F32),
            ),
            in_specs=[away] * 4 + [held] + [away] * 2 + [held] * 4,
            out_specs=(held, held),
            scratch_shapes=scratch,
            compiler_params=pltpu.CompilerParams(
                collective_id=0, has_side_effects=True, vmem_limit_bytes=60 << 20
            ),
        )(
            q, e, s, t, labels[0], first_weights, inner_weights, norm_gain, norm_shift,
            class_weight.T, class_bias[None],
        )
        return (scores[:, :classes].transpose(1, 0, 2)[None], loss[0, 0])

    return per_device


def solution(mesh):
    in_specs = (
        P("batch", "rows", None, None),
        P("batch", "rows", None, None),
        P("batch", "rows", None, None),
        P("batch", "rows", None, None),
        P("batch", "rows", None),
        P(),
        P(),
        P(),
        P(),
        P(),
        P(),
    )
    out_specs = (P("batch", None, "rows", None), P())
    return jax.shard_map(
        make_per_device(dict(mesh.shape)),
        mesh=mesh,
        in_specs=in_specs,
        out_specs=out_specs,
        check_vma=False,
    )
```

```python
import functools

import jax
import jax.numpy as jnp
from jax import lax
from jax.experimental import pallas as pl
from jax.experimental.pallas import tpu as pltpu
from jax.sharding import PartitionSpec as P

GROUPS = 32
NORM_FLOOR = 0.05
IGNORED = 255
Q_CHUNKS = 8
E_CHUNKS = 4
TICKS = (1, 2, 1, 2, 1, 1, 4)
MESH = pl.DeviceIdType.MESH
F32 = jnp.float32
BF16 = jnp.bfloat16


def phase(name):
    pass


def group_fold(x):
    width = x.shape[-1]
    lane = lax.broadcasted_iota(jnp.int32, x.shape, x.ndim - 1)
    step = 1
    while step < width // GROUPS:
        ahead = pltpu.roll(x, width - step, x.ndim - 1)
        behind = pltpu.roll(x, step, x.ndim - 1)
        x = x + jnp.where(lax.rem(lane, 2 * step) < step, ahead, behind)
        step *= 2
    return x


def doubling(rows, cols, source_axis):
    source = lax.broadcasted_iota(jnp.int32, (rows, cols), source_axis)
    target = lax.broadcasted_iota(jnp.int32, (rows, cols), 1 - source_axis)
    count = (rows, cols)[source_axis]
    near = lax.div(target, 2)
    far = jnp.clip(near + 2 * lax.rem(target, 2) - 1, 0, count - 1)
    return (
        0.75 * (source == near).astype(F32) + 0.25 * (source == far).astype(F32)
    ).astype(BF16)


def conv_block(x_ref, flat_ref, start, rows):
    cols, depth = x_ref.shape[1:]
    width = flat_ref.shape[1] // 3
    lhs = jnp.concatenate(
        [
            x_ref[pl.ds(start + down, rows)].reshape(rows * cols, depth)
            for down in range(3)
        ],
        axis=1,
    )
    taps = jnp.dot(lhs, flat_ref[...], preferred_element_type=F32)
    col = lax.rem(lax.broadcasted_iota(jnp.int32, (rows * cols, width), 0), cols)
    left = jnp.where(col == 0, 0.0, pltpu.roll(taps[:, :width], 1, 0))
    right = jnp.where(col == cols - 1, 0.0, pltpu.roll(taps[:, 2 * width :], rows * cols - 1, 0))
    return (taps[:, width : 2 * width] + left + right).reshape(rows, cols, width)


def conv_to(x_ref, flat_ref, y_ref, stat_ref, start, rows, offset):
    y = conv_block(x_ref, flat_ref, start, rows)
    cols = y.shape[1]
    y_ref[pl.ds(start + offset, rows)] = y
    sums = jnp.sum(y, axis=1, keepdims=True)
    centred = y - sums / cols
    stat_ref[pl.ds(start, rows), 0:1] = sums
    stat_ref[pl.ds(start, rows), 1:2] = jnp.sum(centred * centred, axis=1, keepdims=True)


def head_kernel(
    shape,
    q, e, s, t, labels_in, first_w, inner_w, gain_in, shift_in, class_w_in, bias_in,
    out, loss_out,
    labels, gain, shift, class_w, bias,
    q_in, e_in, s_in, t_in, w_q, w_e, w_s, w_t, w_i,
    q_y, e_y, s_y, t_y, s_grown, s_y2, t_grown, t_y2, t_grown2, t_y3,
    t_leave, s_leave, t_leave2, t_land, s_land, t_land2,
    q_stat, e_stat, s_stat, t_stat, s_stat2, t_stat2, t_stat3,
    slab, slabs, class_f, class_pad, up_t, up_s, coarse, wide, scores, loss_slab, loss_slabs,
    local_sem, edge_send, edge_recv, slab_send, slab_recv, loss_send, loss_recv,
):
    size, images = shape["rows"], shape["batch"]
    total = size * images
    me, image = lax.axis_index("rows"), lax.axis_index("batch")
    flat = image * size + me
    width = q_y.shape[2]
    classes = class_w.shape[0]

    def device_at(distance):
        number = lax.rem(flat + distance, total)
        return {"batch": lax.div(number, size), "rows": lax.rem(number, size)}

    phase("enter")
    barrier = pltpu.get_barrier_semaphore()

    def greet(distance, carry):
        pl.semaphore_signal(
            barrier, inc=1, device_id=device_at(distance), device_id_type=MESH
        )
        return carry

    lax.fori_loop(1, total, greet, 0)

    fetched = []

    def fetch(source, target):
        copy = pltpu.make_async_copy(source, target, local_sem.at[len(fetched)])
        copy.start()
        fetched.append(copy)
        return copy

    def fetch_weights(source, target):
        depth = source.shape[2]
        done = local_sem.at[len(fetched)]
        for down in range(3):
            for across in range(3):
                place = target.at[
                    down * depth : (down + 1) * depth, across * width : (across + 1) * width
                ]
                pltpu.make_async_copy(source.at[down, across], place, done).start()
        fetched.append(pltpu.make_async_copy(target, target, done))
        return [fetched[-1]]

    def settle(copies):
        for copy in copies:
            copy.wait()

    q_rows, q_cols = q.shape[:2]
    e_rows, s_rows, t_rows = e.shape[0], s.shape[0], t.shape[0]
    e_cols, s_cols, t_cols = e.shape[1], s.shape[1], t.shape[1]
    got_t = [fetch(t, t_in.at[1 : t_rows + 1])]
    got_s = [fetch(s, s_in.at[1 : s_rows + 1])]
    got_q = fetch_weights(first_w.at[0], w_q) + [fetch(q, q_in.at[1 : q_rows + 1])]
    got_w_t = fetch_weights(first_w.at[3], w_t)
    got_w_s = fetch_weights(first_w.at[2], w_s)
    got_small = [
        fetch(class_w_in, class_w),
        fetch(bias_in, bias),
        fetch(gain_in, gain),
        fetch(shift_in, shift),
        fetch(labels_in, labels),
    ]
    got_i = [fetch_weights(inner_w.at[i], w_i.at[i]) for i in range(3)]
    got_e = fetch_weights(first_w.at[1], w_e) + [fetch(e, e_in.at[1 : e_rows + 1])]

    def exists(offset):
        return me + offset < size if offset > 0 else me + offset >= 0

    def neighbour(offset):
        return {"rows": lax.rem(me + offset + size, size)}

    def edges(lower, upper, before, after, number):
        return [
            (
                pltpu.make_async_remote_copy(
                    src_ref=source,
                    dst_ref=target,
                    send_sem=edge_send.at[number + place],
                    recv_sem=edge_recv.at[number + place],
                    device_id=neighbour(offset),
                    device_id_type=MESH,
                ),
                offset,
            )
            for place, (source, target, offset) in enumerate([(lower, before, 1), (upper, after, -1)])
        ]

    def send(pairs):
        for copy, offset in pairs:
            pl.when(exists(offset))(copy.start)

    def arrive(pairs):
        for copy, offset in pairs:
            pl.when(exists(-offset))(copy.wait_recv)

    def leave(pairs):
        for copy, offset in pairs:
            pl.when(exists(offset))(copy.wait_send)

    def band_edges(field, number):
        last = field.shape[0] - 1
        return edges(field.at[last - 1], field.at[1], field.at[0], field.at[last], number)

    def line_edges(leaving, landing, number):
        return edges(leaving.at[1], leaving.at[0], landing.at[0], landing.at[1], number)

    t_edges, s_edges = band_edges(t_in, 0), band_edges(s_in, 2)
    t_y_edges, s_y_edges = line_edges(t_leave, t_land, 4), line_edges(s_leave, s_land, 6)
    t_y2_edges, coarse_edges = line_edges(t_leave2, t_land2, 8), band_edges(coarse, 10)

    def chunk_edges(source, framed, number, part=slice(None)):
        last = source.shape[0] - 1
        return edges(
            source.at[last, part],
            source.at[0, part],
            framed.at[0, part],
            framed.at[last + 2, part],
            number,
        )

    def parts(cols, count):
        return [pl.ds(k * (cols // count), cols // count) for k in range(count)]

    e_edges, q_edges = chunk_edges(e, e_in, 12), chunk_edges(q, q_in, 14)
    chunks = [chunk_edges(e, e_in, 12, part) for part in parts(e_cols, E_CHUNKS)]
    chunks += [chunk_edges(q, q_in, 14, part) for part in parts(q_cols, Q_CHUNKS)]
    waiting, ticks = list(chunks), list(TICKS)

    def tick():
        for _ in range(ticks.pop(0)):
            send(waiting.pop(0))

    @pl.when(me == 0)
    def _():
        for field in (q_in, e_in, s_in, t_in):
            field[0] = jnp.zeros(field.shape[1:], BF16)

    @pl.when(me == size - 1)
    def _():
        for field in (q_in, e_in, s_in, t_in):
            field[field.shape[0] - 1] = jnp.zeros(field.shape[1:], BF16)

    up_t[...] = doubling(*up_t.shape, 1)
    up_s[...] = doubling(*up_s.shape, 1)

    phase("barrier")
    pl.semaphore_wait(barrier, total - 1)
    phase("send_ts")
    settle(got_t)
    send(t_edges)
    settle(got_s)
    send(s_edges)

    def slab_copy(number, distance, sender):
        return pltpu.make_async_remote_copy(
            src_ref=slab.at[number],
            dst_ref=slabs.at[number, sender],
            send_sem=slab_send.at[number],
            recv_sem=slab_recv.at[number],
            device_id=neighbour(distance),
            device_id_type=MESH,
        )

    def slab_all(number):
        rest = slabs.at[number, 0 : size - 1]
        return pltpu.make_async_remote_copy(
            src_ref=rest,
            dst_ref=rest,
            send_sem=slab_send.at[number],
            recv_sem=slab_recv.at[number],
            device_id=neighbour(1),
            device_id_type=MESH,
        )

    def announce(number, stat, cols):
        rows = stat.shape[0]
        sums = stat[:, 0:1]
        channel = jnp.sum(sums, axis=0)
        mean = group_fold(channel) / (rows * cols * (width // GROUPS))
        strays = sums / cols - mean
        slab[number, 0:1] = channel
        slab[number, 1:2] = jnp.sum(stat[:, 1:2] + cols * (strays * strays), axis=0)
        for distance in range(1, size):
            slab_copy(number, distance, me).start()
        slabs[number, me] = slab[number]

    def gather(number, rows, cols):
        slab_all(number).wait_recv()
        count = rows * cols * (width // GROUPS)
        every = slabs[number].reshape(2 * size, width)
        every = group_fold(every).reshape(size, 2, width)
        means = every[:, 0:1] / count
        mean = jnp.sum(means, axis=0) / size
        strays = means - mean
        squares = jnp.sum(every[:, 1:2] + count * (strays * strays), axis=0)
        return mean, squares / (count * size)

    def activation(stat, layer):
        mean, var = stat
        factor = gain[layer : layer + 1] * lax.rsqrt(var + NORM_FLOOR)
        offset = shift[layer : layer + 1]
        return lambda y: jnp.maximum((y - mean) * factor + offset, 0.0).astype(BF16)

    def part_with(field, leaving, number, pairs):
        own = field.shape[0] - 2
        mean = slab[number, 0:1] / (own * field.shape[1])
        leaving[0] = (field[1] - mean).astype(BF16)
        leaving[1] = (field[own] - mean).astype(BF16)
        send(pairs)

    def frame(field, landing, number, pairs):
        own = field.shape[0] - 2
        arrive(pairs)

        def accept(place, row, sender):
            mean = slabs[number, sender, 0:1] / (own * field.shape[1])
            field[row] = landing[place].astype(F32) + mean

        pl.when(me > 0)(lambda: accept(0, 0, lax.rem(me - 1 + size, size)))
        pl.when(me < size - 1)(lambda: accept(1, own + 1, lax.rem(me + 1, size)))

        @pl.when(me == 0)
        def _():
            field[0] = field[1]

        @pl.when(me == size - 1)
        def _():
            field[own + 1] = field[own]

    def grow(field, grown, up, act):
        own = field.shape[0] - 2
        lines = jnp.concatenate([act(field[row]) for row in range(own + 2)], axis=1)
        lines = jnp.dot(up[...], lines, preferred_element_type=F32)
        for row in range(own + 1):
            here = lines[:, row * width : (row + 1) * width]
            below = lines[:, (row + 1) * width : (row + 2) * width]
            grown[2 * row] = (0.75 * here + 0.25 * below).astype(BF16)
            grown[2 * row + 1] = (0.25 * here + 0.75 * below).astype(BF16)

        @pl.when(me == 0)
        def _():
            grown[0] = jnp.zeros(grown.shape[1:], BF16)

        @pl.when(me == size - 1)
        def _():
            grown[2 * own + 1] = jnp.zeros(grown.shape[1:], BF16)

    def convolve(x_ref, flat_ref, y_ref, stat_ref, offset):
        count, cols = x_ref.shape[0] - 2, x_ref.shape[1]
        rows = max(r for r in range(1, count + 1) if count % r == 0 and (r == 1 or r * cols <= 1024))

        def step(index, carry):
            conv_to(x_ref, flat_ref, y_ref, stat_ref, index * rows, rows, offset)
            return carry

        lax.fori_loop(0, count // rows, step, 0)

    def q_blocks(first, last):
        def step(index, carry):
            conv_to(q_in, w_q, q_y, q_stat, 1 + 2 * index, 2, 0)
            return carry

        lax.fori_loop(first, last, step, 0)

    blocks = (q_rows - 2) // 2
    phase("fetch_q")
    settle(got_q)
    phase("q_blocks_a")
    q_blocks(0, 2)
    tick()
    phase("wait_t")
    settle(got_w_t)
    arrive(t_edges)
    phase("conv_t")
    conv_to(t_in, w_t, t_y, t_stat, 0, t_rows, 1)
    phase("announce_t")
    announce(0, t_stat, t_cols)
    part_with(t_y, t_leave, 0, t_y_edges)
    phase("wait_s")
    settle(got_w_s)
    arrive(s_edges)
    phase("conv_s")
    conv_to(s_in, w_s, s_y, s_stat, 0, s_rows, 1)
    announce(1, s_stat, s_cols)
    part_with(s_y, s_leave, 1, s_y_edges)
    tick()
    phase("q_blocks_b")
    settle(got_small)
    q_blocks(2, 3)
    phase("gather_t")
    norm = gather(0, t_rows, t_cols)
    settle(got_i[1])
    phase("frame_t")
    frame(t_y, t_land, 0, t_y_edges)
    phase("grow_t")
    grow(t_y, t_grown, up_t, activation(norm, 3))
    phase("conv_t2")
    convolve(t_grown, w_i.at[1], t_y2, t_stat2, 1)
    phase("announce_t2")
    announce(2, t_stat2, 2 * t_cols)
    part_with(t_y2, t_leave2, 2, t_y2_edges)
    tick()
    phase("gather_s")
    norm = gather(1, s_rows, s_cols)
    settle(got_i[0])
    phase("frame_s")
    frame(s_y, s_land, 1, s_y_edges)
    phase("grow_s")
    grow(s_y, s_grown, up_s, activation(norm, 2))
    phase("conv_s2")
    convolve(s_grown, w_i.at[0], s_y2, s_stat2, 0)
    announce(3, s_stat2, 2 * s_cols)
    tick()
    phase("q_blocks_c")
    q_blocks(3, 4)
    phase("gather_t2")
    norm = gather(2, 2 * t_rows, 2 * t_cols)
    settle(got_i[2])
    tick()
    phase("frame_t2")
    frame(t_y2, t_land2, 2, t_y2_edges)
    phase("grow_t2")
    grow(t_y2, t_grown2, up_s, activation(norm, 5))
    phase("conv_t3")
    convolve(t_grown2, w_i.at[2], t_y3, t_stat3, 0)
    phase("announce_t3")
    announce(4, t_stat3, 4 * t_cols)
    tick()
    phase("wait_e")
    settle(got_e)
    arrive(e_edges)
    phase("conv_e")
    convolve(e_in, w_e, e_y, e_stat, 0)
    announce(5, e_stat, e_cols)
    tick()
    phase("q_blocks_d")
    q_blocks(4, blocks)
    phase("wait_q")
    arrive(q_edges)
    phase("conv_q_border")

    def border(index, carry):
        conv_to(q_in, w_q, q_y, q_stat, index * (q_rows - 1), 1, 0)
        return carry

    lax.fori_loop(0, 2, border, 0)
    announce(6, q_stat, q_cols)

    phase("gather_t3")
    t_act = activation(gather(4, 4 * t_rows, 4 * t_cols), 6)
    phase("gather_se")
    s_act = activation(gather(3, 2 * s_rows, 2 * s_cols), 4)
    e_act = activation(gather(5, e_rows, e_cols), 1)
    phase("project")
    class_f[...] = jnp.zeros(class_f.shape, F32)
    class_f[0:classes] = class_w[...].astype(F32)
    class_pad[...] = class_f[...].astype(BF16)
    padded = class_f.shape[0]
    weight = class_pad[...]
    weights = jnp.concatenate([weight] * 3, axis=1)
    across = (((1,), (1,)), ((), ()))

    def project(row, carry):
        lines = jnp.concatenate([e_act(e_y[row]), s_act(s_y2[row]), t_act(t_y3[row])], axis=1)
        coarse[row + 1] = lax.dot_general(weights, lines, across, preferred_element_type=F32)
        return carry

    lax.fori_loop(0, e_rows, project, 0, unroll=2)
    send(coarse_edges)

    phase("gather_q")
    q_act = activation(gather(6, q_rows, q_cols), 0)
    spot = lax.broadcasted_iota(jnp.int32, (padded, classes), 0)
    lane = lax.broadcasted_iota(jnp.int32, (padded, classes), 1)
    bias_col = jnp.sum(jnp.where(spot == lane, bias[...], 0.0), axis=1, keepdims=True)
    phase("score_q")

    def score(row, carry):
        scores[row] = (
            lax.dot_general(weight, q_act(q_y[row]), across, preferred_element_type=F32) + bias_col
        )
        return carry

    lax.fori_loop(0, q_rows, score, 0, unroll=4)
    phase("wait_coarse")
    up_cols = doubling(e_cols, q_cols, 0)
    arrive(coarse_edges)

    @pl.when(me == 0)
    def _():
        coarse[0] = coarse[1]

    @pl.when(me == size - 1)
    def _():
        coarse[e_rows + 1] = coarse[e_rows]

    phase("widen")
    lines = coarse[...].reshape((e_rows + 2) * padded, e_cols)
    high = lines.astype(BF16)
    low = (lines - high.astype(F32)).astype(BF16)
    lines = jnp.dot(high, up_cols, preferred_element_type=F32) + jnp.dot(
        low, up_cols, preferred_element_type=F32
    )
    wide[...] = lines.reshape(wide.shape)
    phase("finish")
    kind = lax.broadcasted_iota(jnp.int32, (padded, q_cols), 0)

    def finish(row, grown):
        line = scores[row] + grown
        scores[row] = line
        powers = jnp.where(kind < classes, jnp.exp(line), 0.0)
        log_total = jnp.log(jnp.sum(powers, axis=0, keepdims=True))
        label = labels[pl.ds(row, 1), :]
        picked = jnp.sum(jnp.where(kind == label, line, 0.0), axis=0, keepdims=True)
        usable = label != IGNORED
        return jnp.where(usable, log_total - picked, 0.0), usable.astype(F32)

    def pair(index, carry):
        here = wide[index + 1]
        upper = finish(2 * index, 0.25 * wide[index] + 0.75 * here)
        lower = finish(2 * index + 1, 0.75 * here + 0.25 * wide[index + 2])
        return carry[0] + upper[0] + lower[0], carry[1] + upper[1] + lower[1]

    zero = jnp.zeros((1, q_cols), F32)
    sums = lax.fori_loop(0, e_rows, pair, (zero, zero), unroll=2)
    phase("loss_send")
    for place, line in enumerate(sums):
        loss_slab[place : place + 1] = sum(
            line[:, k * width : (k + 1) * width] for k in range(q_cols // width)
        )

    def loss_copy(source, target, distance):
        return pltpu.make_async_remote_copy(
            src_ref=source,
            dst_ref=target,
            send_sem=loss_send.at[0],
            recv_sem=loss_recv.at[0],
            device_id=device_at(distance),
            device_id_type=MESH,
        )

    def loss_go(distance, carry):
        loss_copy(loss_slab, loss_slabs.at[flat], distance).start()
        return carry

    rest = loss_slabs.at[0 : total - 1]
    loss_all = loss_copy(rest, rest, 1)

    lax.fori_loop(1, total, loss_go, 0)
    loss_slabs[flat] = loss_slab[...]
    phase("output")
    for first in range(0, classes, 8):
        lines = jnp.transpose(scores[:, first : first + 8], (1, 0, 2)).astype(BF16)
        out[first : min(first + 8, classes)] = lines[: min(8, classes - first)]
    phase("leave")
    for pairs in (
        t_edges, s_edges, t_y_edges, s_y_edges, t_y2_edges, coarse_edges, e_edges, q_edges,
    ):
        leave(pairs)
    for number in range(slab.shape[0]):
        slab_all(number).wait_send()
    phase("loss_wait")
    loss_all.wait_recv()
    phase("loss_end")
    ends = jnp.sum(jnp.sum(loss_slabs[...], axis=0), axis=1, keepdims=True)
    loss_out[...] = jnp.broadcast_to(ends[0:1] / jnp.maximum(ends[1:2], 1.0), loss_out.shape)
    loss_all.wait_send()
    phase("")


def make_per_device(shape):
    def per_device(
        feat_quarter,
        feat_eighth,
        feat_sixteenth,
        feat_thirty,
        labels,
        first_weights,
        inner_weights,
        norm_gain,
        norm_shift,
        class_weight,
        class_bias,
    ):
        q, e, s, t = feat_quarter[0], feat_eighth[0], feat_sixteenth[0], feat_thirty[0]
        size = shape["rows"]
        total = size * shape["batch"]
        depth, width = first_weights.shape[3:]
        classes = class_weight.shape[1]
        padded = -(-classes // 8) * 8
        (q_rows, q_cols), (e_rows, e_cols) = q.shape[:2], e.shape[:2]
        (s_rows, s_cols), (t_rows, t_cols) = s.shape[:2], t.shape[:2]

        def framed(rows, cols, channels, kind=BF16):
            return pltpu.VMEM((rows + 2, cols, channels), kind)

        def field(rows, cols):
            return pltpu.VMEM((rows, cols, width), F32)

        def stat(rows):
            return pltpu.VMEM((rows, 8, width), F32)

        def line(cols):
            return pltpu.VMEM((2, cols, width), BF16)

        small = [labels[0], norm_gain, norm_shift, class_weight.T, class_bias[None]]
        scratch = [
            *[pltpu.VMEM(x.shape, x.dtype) for x in small],
            framed(q_rows, q_cols, depth),
            framed(e_rows, e_cols, depth),
            framed(s_rows, s_cols, depth),
            framed(t_rows, t_cols, depth),
            *[pltpu.VMEM((3 * depth, 3 * width), BF16)] * 4,
            pltpu.VMEM((3, 3 * width, 3 * width), BF16),
            field(q_rows, q_cols),
            field(e_rows, e_cols),
            framed(s_rows, s_cols, width, F32),
            framed(t_rows, t_cols, width, F32),
            framed(2 * s_rows, 2 * s_cols, width),
            field(2 * s_rows, 2 * s_cols),
            framed(2 * t_rows, 2 * t_cols, width),
            framed(2 * t_rows, 2 * t_cols, width, F32),
            framed(4 * t_rows, 4 * t_cols, width),
            field(4 * t_rows, 4 * t_cols),
            *[line(cols) for cols in (t_cols, s_cols, 2 * t_cols)] * 2,
            stat(q_rows),
            stat(e_rows),
            stat(s_rows),
            stat(t_rows),
            stat(2 * s_rows),
            stat(2 * t_rows),
            stat(4 * t_rows),
            pltpu.VMEM((7, 2, width), F32),
            pltpu.VMEM((7, size, 2, width), F32),
            pltpu.VMEM((padded, width), F32),
            pltpu.VMEM((padded, width), BF16),
            pltpu.VMEM((2 * t_cols, t_cols), BF16),
            pltpu.VMEM((2 * s_cols, s_cols), BF16),
            framed(e_rows, padded, e_cols, F32),
            framed(e_rows, padded, q_cols, F32),
            pltpu.VMEM((q_rows, padded, q_cols), F32),
            pltpu.VMEM((2, width), F32),
            pltpu.VMEM((total, 2, width), F32),
            *[pltpu.SemaphoreType.DMA((count,)) for count in (17, 16, 16, 7, 7, 1, 1)],
        ]
        away, held = pl.BlockSpec(memory_space=pl.ANY), pl.BlockSpec(memory_space=pltpu.VMEM)
        operands = (q, e, s, t, small[0], first_weights, inner_weights, *small[1:])
        logits, loss = pl.pallas_call(
            functools.partial(head_kernel, shape),
            out_shape=(
                jax.ShapeDtypeStruct((classes, q_rows, q_cols), BF16),
                jax.ShapeDtypeStruct((8, width), F32),
            ),
            in_specs=[away] * 11,
            out_specs=(held, held),
            scratch_shapes=scratch,
            compiler_params=pltpu.CompilerParams(
                collective_id=0, has_side_effects=True, vmem_limit_bytes=32 << 20
            ),
        )(*[pltpu.with_memory_space_constraint(x, pltpu.HBM) for x in operands])
        return (logits[None], loss[0, 0])

    return per_device


def solution(mesh):
    in_specs = (
        P("batch", "rows", None, None),
        P("batch", "rows", None, None),
        P("batch", "rows", None, None),
        P("batch", "rows", None, None),
        P("batch", "rows", None),
        P(),
        P(),
        P(),
        P(),
        P(),
        P(),
    )
    out_specs = (P("batch", None, "rows", None), P())
    return jax.shard_map(
        make_per_device(dict(mesh.shape)),
        mesh=mesh,
        in_specs=in_specs,
        out_specs=out_specs,
        check_vma=False,
    )
```

```python
import functools

import jax
import jax.numpy as jnp
from jax import lax
from jax.experimental import pallas as pl
from jax.experimental.pallas import tpu as pltpu
from jax.sharding import PartitionSpec as P

GROUPS = 32
NORM_FLOOR = 0.05
IGNORED = 255
Q_CHUNKS = 4
E_CHUNKS = 2
TICKS = (1, 1, 1, 1, 1, 1)
PAIRS = (3, 2, 1, 2)
MESH = pl.DeviceIdType.MESH
F32 = jnp.float32
BF16 = jnp.bfloat16


def phase(name):
    pass


def group_fold(x):
    width = x.shape[-1]
    lane = lax.broadcasted_iota(jnp.int32, x.shape, x.ndim - 1)
    step = 1
    while step < width // GROUPS:
        ahead = pltpu.roll(x, width - step, x.ndim - 1)
        behind = pltpu.roll(x, step, x.ndim - 1)
        x = x + jnp.where(lax.rem(lane, 2 * step) < step, ahead, behind)
        step *= 2
    return x


def doubling(rows, cols, source_axis):
    source = lax.broadcasted_iota(jnp.int32, (rows, cols), source_axis)
    target = lax.broadcasted_iota(jnp.int32, (rows, cols), 1 - source_axis)
    count = (rows, cols)[source_axis]
    near = lax.div(target, 2)
    far = jnp.clip(near + 2 * lax.rem(target, 2) - 1, 0, count - 1)
    return (
        0.75 * (source == near).astype(F32) + 0.25 * (source == far).astype(F32)
    ).astype(BF16)


def conv_block(lines, flat, rows):
    width = flat.shape[1] // 3
    count = lines.shape[0]
    cols = count // rows
    taps = jnp.dot(lines, flat, preferred_element_type=F32)
    col = lax.rem(lax.broadcasted_iota(jnp.int32, (count, width), 0), cols)
    left = jnp.where(col == 0, 0.0, pltpu.roll(taps[:, :width], 1, 0))
    right = jnp.where(col == cols - 1, 0.0, pltpu.roll(taps[:, 2 * width :], count - 1, 0))
    return (taps[:, width : 2 * width] + left + right).reshape(rows, cols, width)


def keep(y, y_ref, stat_ref, start, offset):
    rows, cols = y.shape[:2]
    y_ref[pl.ds(start + offset, rows)] = y
    sums = jnp.sum(y, axis=1, keepdims=True)
    centred = y - sums / cols
    stat_ref[pl.ds(start, rows), 0:1] = sums
    stat_ref[pl.ds(start, rows), 1:2] = jnp.sum(centred * centred, axis=1, keepdims=True)


def conv_to(x_ref, flat_ref, y_ref, stat_ref, start, rows, offset):
    cols, depth = x_ref.shape[1:]
    lines = [
        x_ref[pl.ds(start + down, rows)].reshape(rows * cols, depth) for down in range(3)
    ]
    y = conv_block(jnp.concatenate(lines, axis=1), flat_ref[...], rows)
    keep(y, y_ref, stat_ref, start, offset)


def head_kernel(
    shape,
    q, e, s, t, labels_in, first_w, inner_w, gain_in, shift_in, class_w_in, bias_in,
    out, loss_out,
    labels, gain, shift, class_w, bias,
    q_in, e_in, s_in, t_in, w_q, w_e, w_s, w_t, w_i,
    q_y, e_y, s_y, t_y, s_grown, s_y2, t_grown, t_y2, t_grown2, t_y3,
    t_leave, s_leave, t_leave2, e_leave, q_leave, t_land, s_land, t_land2, e_land, q_land,
    base_leave, base_land,
    q_stat, e_stat, s_stat, t_stat, s_stat2, t_stat2, t_stat3,
    slab, slabs, class_f, class_pad, up_t, up_s, coarse, wide, scores, loss_slab, loss_slabs,
    local_sem, edge_send, edge_recv, slab_send, slab_recv, loss_send, loss_recv,
):
    size, images = shape["rows"], shape["batch"]
    total = size * images
    me, image = lax.axis_index("rows"), lax.axis_index("batch")
    flat = image * size + me
    width = q_y.shape[2]
    classes = class_w.shape[0]

    def device_at(distance):
        number = lax.rem(flat + distance, total)
        return {"batch": lax.div(number, size), "rows": lax.rem(number, size)}

    phase("enter")
    barrier = pltpu.get_barrier_semaphore()

    def greet(distance, carry):
        pl.semaphore_signal(
            barrier, inc=1, device_id=device_at(distance), device_id_type=MESH
        )
        return carry

    lax.fori_loop(1, total, greet, 0)

    fetched = []

    def fetch(source, target):
        copy = pltpu.make_async_copy(source, target, local_sem.at[len(fetched)])
        copy.start()
        fetched.append(copy)
        return copy

    def fetch_weights(source, target):
        depth = source.shape[2]
        done = local_sem.at[len(fetched)]
        for down in range(3):
            for across in range(3):
                place = target.at[
                    down * depth : (down + 1) * depth, across * width : (across + 1) * width
                ]
                pltpu.make_async_copy(source.at[down, across], place, done).start()
        fetched.append(pltpu.make_async_copy(target, target, done))
        return [fetched[-1]]

    def settle(copies):
        for copy in copies:
            copy.wait()

    q_rows, q_cols = q.shape[:2]
    e_rows, s_rows, t_rows = e.shape[0], s.shape[0], t.shape[0]
    e_cols, s_cols, t_cols = e.shape[1], s.shape[1], t.shape[1]
    got_t = [fetch(t, t_in.at[1 : t_rows + 1])]
    got_s = [fetch(s, s_in.at[1 : s_rows + 1])]
    got_q = fetch_weights(first_w.at[0], w_q) + [fetch(q, q_in.at[1 : q_rows + 1])]
    got_w_t = fetch_weights(first_w.at[3], w_t)
    got_w_s = fetch_weights(first_w.at[2], w_s)
    got_small = [
        fetch(class_w_in, class_w),
        fetch(bias_in, bias),
        fetch(gain_in, gain),
        fetch(shift_in, shift),
        fetch(labels_in, labels),
    ]
    got_i = [fetch_weights(inner_w.at[i], w_i.at[i]) for i in range(3)]
    got_e = fetch_weights(first_w.at[1], w_e) + [fetch(e, e_in.at[1 : e_rows + 1])]

    def exists(offset):
        return me + offset < size if offset > 0 else me + offset >= 0

    def neighbour(offset):
        return {"rows": lax.rem(me + offset + size, size)}

    def edges(lower, upper, before, after, number):
        return [
            (
                pltpu.make_async_remote_copy(
                    src_ref=source,
                    dst_ref=target,
                    send_sem=edge_send.at[number + place],
                    recv_sem=edge_recv.at[number + place],
                    device_id=neighbour(offset),
                    device_id_type=MESH,
                ),
                offset,
            )
            for place, (source, target, offset) in enumerate([(lower, before, 1), (upper, after, -1)])
        ]

    def send(pairs):
        for copy, offset in pairs:
            pl.when(exists(offset))(copy.start)

    def arrive(pairs):
        for copy, offset in pairs:
            pl.when(exists(-offset))(copy.wait_recv)

    def leave(pairs):
        for copy, offset in pairs:
            pl.when(exists(offset))(copy.wait_send)

    def band_edges(field, number):
        last = field.shape[0] - 1
        return edges(field.at[last - 1], field.at[1], field.at[0], field.at[last], number)

    def line_edges(leaving, landing, number):
        return edges(leaving.at[1], leaving.at[0], landing.at[0], landing.at[1], number)

    t_edges, s_edges = band_edges(t_in, 0), band_edges(s_in, 2)
    t_y_edges, s_y_edges = line_edges(t_leave, t_land, 4), line_edges(s_leave, s_land, 6)
    t_y2_edges, coarse_edges = line_edges(t_leave2, t_land2, 8), band_edges(coarse, 10)

    def part_edges(leaving, landing, number, chunks):
        step = leaving.shape[1] // chunks
        return [
            edges(
                leaving.at[1, part], leaving.at[0, part], landing.at[0, part], landing.at[1, part], number
            )
            for part in (pl.ds(k * step, step) for k in range(chunks))
        ]

    e_edges, q_edges = line_edges(e_leave, e_land, 12), line_edges(q_leave, q_land, 14)
    base_edges = line_edges(base_leave, base_land, 16)
    chunks = part_edges(e_leave, e_land, 12, E_CHUNKS) + part_edges(q_leave, q_land, 14, Q_CHUNKS)
    waiting, ticks = list(chunks), list(TICKS)

    def tick():
        for _ in range(ticks.pop(0)):
            send(waiting.pop(0))

    @pl.when(me == 0)
    def _():
        for field in (s_in, t_in):
            field[0] = jnp.zeros(field.shape[1:], BF16)

    @pl.when(me == size - 1)
    def _():
        for field in (s_in, t_in):
            field[field.shape[0] - 1] = jnp.zeros(field.shape[1:], BF16)

    for field in (q_in, e_in):
        for row in (0, field.shape[0] - 1):
            field[row] = jnp.zeros(field.shape[1:], BF16)

    up_t[...] = doubling(*up_t.shape, 1)
    up_s[...] = doubling(*up_s.shape, 1)

    phase("barrier")
    pl.semaphore_wait(barrier, total - 1)
    phase("send_ts")
    settle(got_t)
    send(t_edges)

    def slab_copy(number, distance, sender):
        return pltpu.make_async_remote_copy(
            src_ref=slab.at[number],
            dst_ref=slabs.at[number, sender],
            send_sem=slab_send.at[number],
            recv_sem=slab_recv.at[number],
            device_id=neighbour(distance),
            device_id_type=MESH,
        )

    def slab_all(number):
        rest = slabs.at[number, 0 : size - 1]
        return pltpu.make_async_remote_copy(
            src_ref=rest,
            dst_ref=rest,
            send_sem=slab_send.at[number],
            recv_sem=slab_recv.at[number],
            device_id=neighbour(1),
            device_id_type=MESH,
        )

    def announce(number, stat, cols):
        rows = stat.shape[0]
        sums = stat[:, 0:1]
        channel = jnp.sum(sums, axis=0)
        mean = group_fold(channel) / (rows * cols * (width // GROUPS))
        strays = sums / cols - mean
        slab[number, 0:1] = channel
        slab[number, 1:2] = jnp.sum(stat[:, 1:2] + cols * (strays * strays), axis=0)
        for distance in range(1, size):
            slab_copy(number, distance, me).start()
        slabs[number, me] = slab[number]

    def gather(number, rows, cols):
        slab_all(number).wait_recv()
        count = rows * cols * (width // GROUPS)
        every = slabs[number].reshape(2 * size, width)
        every = group_fold(every).reshape(size, 2, width)
        means = every[:, 0:1] / count
        mean = jnp.sum(means, axis=0) / size
        strays = means - mean
        squares = jnp.sum(every[:, 1:2] + count * (strays * strays), axis=0)
        return mean, squares / (count * size)

    def activation(stat, layer):
        mean, var = stat
        factor = gain[layer : layer + 1] * lax.rsqrt(var + NORM_FLOOR)
        offset = shift[layer : layer + 1]
        return lambda y: jnp.maximum((y - mean) * factor + offset, 0.0).astype(BF16)

    def part_with(field, leaving, number, pairs):
        own = field.shape[0] - 2
        mean = slab[number, 0:1] / (own * field.shape[1])
        leaving[0] = (field[1] - mean).astype(BF16)
        leaving[1] = (field[own] - mean).astype(BF16)
        send(pairs)

    def frame(field, landing, number, pairs):
        own = field.shape[0] - 2
        arrive(pairs)

        def accept(place, row, sender):
            mean = slabs[number, sender, 0:1] / (own * field.shape[1])
            field[row] = landing[place].astype(F32) + mean

        pl.when(me > 0)(lambda: accept(0, 0, lax.rem(me - 1 + size, size)))
        pl.when(me < size - 1)(lambda: accept(1, own + 1, lax.rem(me + 1, size)))

        @pl.when(me == 0)
        def _():
            field[0] = field[1]

        @pl.when(me == size - 1)
        def _():
            field[own + 1] = field[own]

    def grow(field, grown, up, act):
        own = field.shape[0] - 2
        lines = jnp.concatenate([act(field[row]) for row in range(own + 2)], axis=1)
        lines = jnp.dot(up[...], lines, preferred_element_type=F32)
        for row in range(own + 1):
            here = lines[:, row * width : (row + 1) * width]
            below = lines[:, (row + 1) * width : (row + 2) * width]
            grown[2 * row] = (0.75 * here + 0.25 * below).astype(BF16)
            grown[2 * row + 1] = (0.25 * here + 0.75 * below).astype(BF16)

        @pl.when(me == 0)
        def _():
            grown[0] = jnp.zeros(grown.shape[1:], BF16)

        @pl.when(me == size - 1)
        def _():
            grown[2 * own + 1] = jnp.zeros(grown.shape[1:], BF16)

    def convolve(x_ref, flat_ref, y_ref, stat_ref, offset):
        count, cols = x_ref.shape[0] - 2, x_ref.shape[1]
        rows = max(r for r in range(1, count + 1) if count % r == 0 and (r == 1 or r * cols <= 1024))

        def step(index, carry):
            conv_to(x_ref, flat_ref, y_ref, stat_ref, index * rows, rows, offset)
            return carry

        lax.fori_loop(0, count // rows, step, 0)

    done, pairs_left = [0], list(PAIRS)

    def q_blocks():
        first, last = done[0], done[0] + pairs_left.pop(0)
        done[0] = last = last if pairs_left else q_rows // 2

        def step(index, carry):
            conv_to(q_in, w_q, q_y, q_stat, 2 * index, 2, 0)
            return carry

        lax.fori_loop(first, last, step, 0)

    def lend(x_ref, flat_ref, leaving, place):
        depth, last = x_ref.shape[2], x_ref.shape[0] - 2
        for side, row, down in ((0, 1, 2), (1, last, 0)):
            flat = flat_ref[down * depth : (down + 1) * depth]
            term = conv_block(x_ref[row], flat, 1)[0]
            base = jnp.sum(term, axis=0, keepdims=True) / term.shape[0]
            leaving[side] = (term - base).astype(BF16)
            base_leave[side, place : place + 1] = base

    def mend(y_ref, stat_ref, landing, place, pairs):
        arrive(pairs)

        def add(side, row):
            term = landing[side].astype(F32) + base_land[side, place : place + 1]
            keep((y_ref[row] + term)[None], y_ref, stat_ref, row, 0)

        pl.when(me > 0)(lambda: add(0, 0))
        pl.when(me < size - 1)(lambda: add(1, y_ref.shape[0] - 1))

    phase("fetch_q")
    settle(got_q)
    phase("lend_q")
    lend(q_in, w_q, q_leave, 0)
    settle(got_s)
    send(s_edges)
    phase("q_blocks_a")
    q_blocks()
    phase("lend_e")
    settle(got_e)
    lend(e_in, w_e, e_leave, 1)
    send(base_edges)
    tick()
    phase("wait_t")
    settle(got_w_t)
    arrive(t_edges)
    phase("conv_t")
    conv_to(t_in, w_t, t_y, t_stat, 0, t_rows, 1)
    phase("announce_t")
    announce(0, t_stat, t_cols)
    part_with(t_y, t_leave, 0, t_y_edges)
    phase("wait_s")
    settle(got_w_s)
    arrive(s_edges)
    phase("conv_s")
    conv_to(s_in, w_s, s_y, s_stat, 0, s_rows, 1)
    announce(1, s_stat, s_cols)
    part_with(s_y, s_leave, 1, s_y_edges)
    tick()
    phase("q_blocks_b")
    settle(got_small)
    q_blocks()
    phase("gather_t")
    norm = gather(0, t_rows, t_cols)
    settle(got_i[1])
    phase("frame_t")
    frame(t_y, t_land, 0, t_y_edges)
    phase("grow_t")
    grow(t_y, t_grown, up_t, activation(norm, 3))
    phase("conv_t2")
    convolve(t_grown, w_i.at[1], t_y2, t_stat2, 1)
    phase("announce_t2")
    announce(2, t_stat2, 2 * t_cols)
    part_with(t_y2, t_leave2, 2, t_y2_edges)
    tick()
    phase("gather_s")
    norm = gather(1, s_rows, s_cols)
    settle(got_i[0])
    phase("frame_s")
    frame(s_y, s_land, 1, s_y_edges)
    phase("grow_s")
    grow(s_y, s_grown, up_s, activation(norm, 2))
    phase("conv_s2")
    convolve(s_grown, w_i.at[0], s_y2, s_stat2, 0)
    announce(3, s_stat2, 2 * s_cols)
    tick()
    phase("q_blocks_c")
    q_blocks()
    phase("gather_t2")
    norm = gather(2, 2 * t_rows, 2 * t_cols)
    settle(got_i[2])
    tick()
    phase("frame_t2")
    frame(t_y2, t_land2, 2, t_y2_edges)
    phase("grow_t2")
    grow(t_y2, t_grown2, up_s, activation(norm, 5))
    phase("conv_t3")
    convolve(t_grown2, w_i.at[2], t_y3, t_stat3, 0)
    phase("announce_t3")
    announce(4, t_stat3, 4 * t_cols)
    tick()
    phase("wait_e")
    convolve(e_in, w_e, e_y, e_stat, 0)
    arrive(base_edges)
    phase("mend_e")
    mend(e_y, e_stat, e_land, 1, e_edges)
    announce(5, e_stat, e_cols)
    phase("q_blocks_d")
    q_blocks()
    phase("mend_q")
    mend(q_y, q_stat, q_land, 0, q_edges)
    announce(6, q_stat, q_cols)

    phase("gather_t3")
    t_act = activation(gather(4, 4 * t_rows, 4 * t_cols), 6)
    phase("gather_se")
    s_act = activation(gather(3, 2 * s_rows, 2 * s_cols), 4)
    e_act = activation(gather(5, e_rows, e_cols), 1)
    phase("project")
    class_f[...] = jnp.zeros(class_f.shape, F32)
    class_f[0:classes] = class_w[...].astype(F32)
    class_pad[...] = class_f[...].astype(BF16)
    padded = class_f.shape[0]
    weight = class_pad[...]
    weights = jnp.concatenate([weight] * 3, axis=1)
    across = (((1,), (1,)), ((), ()))

    def project(row, carry):
        lines = jnp.concatenate([e_act(e_y[row]), s_act(s_y2[row]), t_act(t_y3[row])], axis=1)
        coarse[row + 1] = lax.dot_general(weights, lines, across, preferred_element_type=F32)
        return carry

    lax.fori_loop(0, e_rows, project, 0, unroll=2)
    send(coarse_edges)

    phase("gather_q")
    q_act = activation(gather(6, q_rows, q_cols), 0)
    spot = lax.broadcasted_iota(jnp.int32, (padded, classes), 0)
    lane = lax.broadcasted_iota(jnp.int32, (padded, classes), 1)
    bias_col = jnp.sum(jnp.where(spot == lane, bias[...], 0.0), axis=1, keepdims=True)
    phase("score_q")

    def score(row, carry):
        scores[row] = (
            lax.dot_general(weight, q_act(q_y[row]), across, preferred_element_type=F32) + bias_col
        )
        return carry

    lax.fori_loop(0, q_rows, score, 0, unroll=4)
    phase("wait_coarse")
    up_cols = doubling(e_cols, q_cols, 0)
    arrive(coarse_edges)

    @pl.when(me == 0)
    def _():
        coarse[0] = coarse[1]

    @pl.when(me == size - 1)
    def _():
        coarse[e_rows + 1] = coarse[e_rows]

    phase("widen")
    lines = coarse[...].reshape((e_rows + 2) * padded, e_cols)
    high = lines.astype(BF16)
    low = (lines - high.astype(F32)).astype(BF16)
    lines = jnp.dot(high, up_cols, preferred_element_type=F32) + jnp.dot(
        low, up_cols, preferred_element_type=F32
    )
    wide[...] = lines.reshape(wide.shape)
    phase("finish")
    kind = lax.broadcasted_iota(jnp.int32, (padded, q_cols), 0)

    def finish(row, grown):
        line = scores[row] + grown
        scores[row] = line
        powers = jnp.where(kind < classes, jnp.exp(line), 0.0)
        log_total = jnp.log(jnp.sum(powers, axis=0, keepdims=True))
        label = labels[pl.ds(row, 1), :]
        picked = jnp.sum(jnp.where(kind == label, line, 0.0), axis=0, keepdims=True)
        usable = label != IGNORED
        return jnp.where(usable, log_total - picked, 0.0), usable.astype(F32)

    def pair(index, carry):
        here = wide[index + 1]
        upper = finish(2 * index, 0.25 * wide[index] + 0.75 * here)
        lower = finish(2 * index + 1, 0.75 * here + 0.25 * wide[index + 2])
        return carry[0] + upper[0] + lower[0], carry[1] + upper[1] + lower[1]

    zero = jnp.zeros((1, q_cols), F32)
    sums = lax.fori_loop(0, e_rows, pair, (zero, zero), unroll=2)
    phase("loss_send")
    for place, line in enumerate(sums):
        loss_slab[place : place + 1] = sum(
            line[:, k * width : (k + 1) * width] for k in range(q_cols // width)
        )

    def loss_copy(source, target, distance):
        return pltpu.make_async_remote_copy(
            src_ref=source,
            dst_ref=target,
            send_sem=loss_send.at[0],
            recv_sem=loss_recv.at[0],
            device_id=device_at(distance),
            device_id_type=MESH,
        )

    def loss_go(distance, carry):
        loss_copy(loss_slab, loss_slabs.at[flat], distance).start()
        return carry

    rest = loss_slabs.at[0 : total - 1]
    loss_all = loss_copy(rest, rest, 1)

    lax.fori_loop(1, total, loss_go, 0)
    loss_slabs[flat] = loss_slab[...]
    phase("output")
    for first in range(0, classes, 8):
        lines = jnp.transpose(scores[:, first : first + 8], (1, 0, 2)).astype(BF16)
        out[first : min(first + 8, classes)] = lines[: min(8, classes - first)]
    phase("leave")
    for pairs in (
        t_edges, s_edges, t_y_edges, s_y_edges, t_y2_edges, coarse_edges, e_edges, q_edges, base_edges,
    ):
        leave(pairs)
    for number in range(slab.shape[0]):
        slab_all(number).wait_send()
    phase("loss_wait")
    loss_all.wait_recv()
    phase("loss_end")
    ends = jnp.sum(jnp.sum(loss_slabs[...], axis=0), axis=1, keepdims=True)
    loss_out[...] = jnp.broadcast_to(ends[0:1] / jnp.maximum(ends[1:2], 1.0), loss_out.shape)
    loss_all.wait_send()
    phase("")


def make_per_device(shape):
    def per_device(
        feat_quarter,
        feat_eighth,
        feat_sixteenth,
        feat_thirty,
        labels,
        first_weights,
        inner_weights,
        norm_gain,
        norm_shift,
        class_weight,
        class_bias,
    ):
        q, e, s, t = feat_quarter[0], feat_eighth[0], feat_sixteenth[0], feat_thirty[0]
        size = shape["rows"]
        total = size * shape["batch"]
        depth, width = first_weights.shape[3:]
        classes = class_weight.shape[1]
        padded = -(-classes // 8) * 8
        (q_rows, q_cols), (e_rows, e_cols) = q.shape[:2], e.shape[:2]
        (s_rows, s_cols), (t_rows, t_cols) = s.shape[:2], t.shape[:2]

        def framed(rows, cols, channels, kind=BF16):
            return pltpu.VMEM((rows + 2, cols, channels), kind)

        def field(rows, cols):
            return pltpu.VMEM((rows, cols, width), F32)

        def stat(rows):
            return pltpu.VMEM((rows, 8, width), F32)

        def line(cols):
            return pltpu.VMEM((2, cols, width), BF16)

        small = [labels[0], norm_gain, norm_shift, class_weight.T, class_bias[None]]
        scratch = [
            *[pltpu.VMEM(x.shape, x.dtype) for x in small],
            framed(q_rows, q_cols, depth),
            framed(e_rows, e_cols, depth),
            framed(s_rows, s_cols, depth),
            framed(t_rows, t_cols, depth),
            *[pltpu.VMEM((3 * depth, 3 * width), BF16)] * 4,
            pltpu.VMEM((3, 3 * width, 3 * width), BF16),
            field(q_rows, q_cols),
            field(e_rows, e_cols),
            framed(s_rows, s_cols, width, F32),
            framed(t_rows, t_cols, width, F32),
            framed(2 * s_rows, 2 * s_cols, width),
            field(2 * s_rows, 2 * s_cols),
            framed(2 * t_rows, 2 * t_cols, width),
            framed(2 * t_rows, 2 * t_cols, width, F32),
            framed(4 * t_rows, 4 * t_cols, width),
            field(4 * t_rows, 4 * t_cols),
            *[line(cols) for cols in (t_cols, s_cols, 2 * t_cols, e_cols, q_cols)] * 2,
            *[pltpu.VMEM((2, 2, width), F32)] * 2,
            stat(q_rows),
            stat(e_rows),
            stat(s_rows),
            stat(t_rows),
            stat(2 * s_rows),
            stat(2 * t_rows),
            stat(4 * t_rows),
            pltpu.VMEM((7, 2, width), F32),
            pltpu.VMEM((7, size, 2, width), F32),
            pltpu.VMEM((padded, width), F32),
            pltpu.VMEM((padded, width), BF16),
            pltpu.VMEM((2 * t_cols, t_cols), BF16),
            pltpu.VMEM((2 * s_cols, s_cols), BF16),
            framed(e_rows, padded, e_cols, F32),
            framed(e_rows, padded, q_cols, F32),
            pltpu.VMEM((q_rows, padded, q_cols), F32),
            pltpu.VMEM((2, width), F32),
            pltpu.VMEM((total, 2, width), F32),
            *[pltpu.SemaphoreType.DMA((count,)) for count in (17, 18, 18, 7, 7, 1, 1)],
        ]
        away, held = pl.BlockSpec(memory_space=pl.ANY), pl.BlockSpec(memory_space=pltpu.VMEM)
        operands = (q, e, s, t, small[0], first_weights, inner_weights, *small[1:])
        logits, loss = pl.pallas_call(
            functools.partial(head_kernel, shape),
            out_shape=(
                jax.ShapeDtypeStruct((classes, q_rows, q_cols), BF16),
                jax.ShapeDtypeStruct((8, width), F32),
            ),
            in_specs=[away] * 11,
            out_specs=(held, held),
            scratch_shapes=scratch,
            compiler_params=pltpu.CompilerParams(
                collective_id=0, has_side_effects=True, vmem_limit_bytes=32 << 20
            ),
        )(*[pltpu.with_memory_space_constraint(x, pltpu.HBM) for x in operands])
        return (logits[None], loss[0, 0])

    return per_device


def solution(mesh):
    in_specs = (
        P("batch", "rows", None, None),
        P("batch", "rows", None, None),
        P("batch", "rows", None, None),
        P("batch", "rows", None, None),
        P("batch", "rows", None),
        P(),
        P(),
        P(),
        P(),
        P(),
        P(),
    )
    out_specs = (P("batch", None, "rows", None), P())
    return jax.shard_map(
        make_per_device(dict(mesh.shape)),
        mesh=mesh,
        in_specs=in_specs,
        out_specs=out_specs,
        check_vma=False,
    )
```

```python
import functools

import jax
import jax.numpy as jnp
from jax import lax
from jax.experimental import pallas as pl
from jax.experimental.pallas import tpu as pltpu
from jax.sharding import PartitionSpec as P

GROUPS = 32
NORM_FLOOR = 0.05
IGNORED = 255
Q_CHUNKS = 4
E_CHUNKS = 2
TICKS = (2, 0, 0, 0, 0, 1, 0, 0, 0, 0, 2, 1, 0)
PAIRS = (4, 4, 0)
MESH = pl.DeviceIdType.MESH
F32 = jnp.float32
BF16 = jnp.bfloat16


def phase(name):
    pass


def group_fold(x):
    width = x.shape[-1]
    lane = lax.broadcasted_iota(jnp.int32, x.shape, x.ndim - 1)
    step = 1
    while step < width // GROUPS:
        ahead = pltpu.roll(x, width - step, x.ndim - 1)
        behind = pltpu.roll(x, step, x.ndim - 1)
        x = x + jnp.where(lax.rem(lane, 2 * step) < step, ahead, behind)
        step *= 2
    return x


def doubling(rows, cols, source_axis):
    source = lax.broadcasted_iota(jnp.int32, (rows, cols), source_axis)
    target = lax.broadcasted_iota(jnp.int32, (rows, cols), 1 - source_axis)
    count = (rows, cols)[source_axis]
    near = lax.div(target, 2)
    far = jnp.clip(near + 2 * lax.rem(target, 2) - 1, 0, count - 1)
    return (
        0.75 * (source == near).astype(F32) + 0.25 * (source == far).astype(F32)
    ).astype(BF16)


def from_left(taps, cols):
    col = lax.rem(lax.broadcasted_iota(jnp.int32, taps.shape, 0), cols)
    return jnp.where(col == 0, 0.0, pltpu.roll(taps, 1, 0))


def from_right(taps, cols):
    count = taps.shape[0]
    col = lax.rem(lax.broadcasted_iota(jnp.int32, taps.shape, 0), cols)
    return jnp.where(col == cols - 1, 0.0, pltpu.roll(taps, count - 1, 0))


def keep(y, y_ref, stat_ref, row, offset):
    y_ref[row + offset] = y
    sums = jnp.sum(y, axis=0, keepdims=True)
    centred = y - sums / y.shape[0]
    stat_ref[row, 0:1] = sums
    stat_ref[row, 1:2] = jnp.sum(centred * centred, axis=0, keepdims=True)


def conv_to(x_ref, weights, y_ref, stat_ref, start, pairs, offset):
    flat, both = weights
    cols, depth = x_ref.shape[1:]
    width = flat.shape[1] // 3
    lines = jnp.concatenate(
        [
            jnp.concatenate([x_ref[start + 2 * k + down] for k in range(pairs)], axis=0)
            for down in range(4)
        ],
        axis=1,
    )
    first = jnp.dot(lines[:, : 3 * depth], flat[:, : 2 * width], preferred_element_type=F32)
    shared = jnp.dot(lines, both[...], preferred_element_type=F32)
    last = jnp.dot(lines[:, depth:], flat[:, width:], preferred_element_type=F32)
    upper = first[:, width:] + from_left(first[:, :width], cols) + from_right(shared[:, :width], cols)
    lower = last[:, :width] + from_left(shared[:, width:], cols) + from_right(last[:, width:], cols)
    for k in range(pairs):
        for row, y in ((0, upper), (1, lower)):
            keep(y[k * cols : (k + 1) * cols], y_ref, stat_ref, start + 2 * k + row, offset)


def border_term(line, flat):
    width = flat.shape[1] // 3
    taps = jnp.dot(line, flat, preferred_element_type=F32)
    cols = line.shape[0]
    return (
        taps[:, width : 2 * width]
        + from_left(taps[:, :width], cols)
        + from_right(taps[:, 2 * width :], cols)
    )


def head_kernel(
    shape,
    q, e, s, t, labels_in, first_w, inner_w, gain_in, shift_in, class_w_in, bias_in,
    out, loss_out,
    labels, gain, shift, class_w, bias,
    q_in, e_in, s_in, t_in, w_q, w_e, w_s, w_t, w_i, b_q, b_e, b_s, b_t, b_i,
    q_y, e_y, s_y, t_y, s_grown, s_y2, t_grown, t_y2, t_grown2, t_y3,
    t_leave, s_leave, t_leave2, t_leave3, t_lent, s_lent, e_lent, q_lent,
    t_land, s_land, t_land2, t_land3, t_owed, s_owed, e_owed, q_owed,
    base_leave, base_land,
    q_stat, e_stat, s_stat, t_stat, s_stat2, t_stat2, t_stat3,
    slab, slabs, class_f, class_pad, up_t, up_s, coarse, wide, scores, loss_slab, loss_slabs,
    local_sem, edge_send, edge_recv, slab_send, slab_recv, loss_send, loss_recv,
):
    size, images = shape["rows"], shape["batch"]
    total = size * images
    me, image = lax.axis_index("rows"), lax.axis_index("batch")
    flat = image * size + me
    width = q_y.shape[2]
    classes = class_w.shape[0]

    def wrapped(place, distance, count):
        place = place + distance
        return jnp.where(place >= count, place - count, place)

    peers = [
        {"batch": wrapped(image, across, images), "rows": wrapped(me, along, size)}
        for across in range(images)
        for along in range(size)
        if across or along
    ]

    phase("enter")
    barrier = pltpu.get_barrier_semaphore()
    for peer in peers:
        pl.semaphore_signal(barrier, inc=1, device_id=peer, device_id_type=MESH)

    fetched = []

    def fetch(source, target):
        copy = pltpu.make_async_copy(source, target, local_sem.at[len(fetched)])
        copy.start()
        fetched.append(copy)
        return copy

    def block(ref, down, column):
        depth = ref.shape[0] // (3 if ref.shape[1] == 3 * width else 4)
        return ref.at[down * depth : (down + 1) * depth, column * width : (column + 1) * width]

    def fetch_flat(source, target):
        done = local_sem.at[len(fetched)]
        for down in range(3):
            for across in range(3):
                place = block(target, down, across)
                pltpu.make_async_copy(source.at[down, across], place, done).start()
        fetched.append(pltpu.make_async_copy(target, target, done))
        return fetched[-1:]

    def fetch_both(source, target):
        done = local_sem.at[len(fetched)]
        for down in range(3):
            pltpu.make_async_copy(source.at[down, 2], block(target, down, 0), done).start()
            pltpu.make_async_copy(source.at[down, 0], block(target, down + 1, 1), done).start()
        part = target.at[0 : 3 * source.shape[2]]
        fetched.append(pltpu.make_async_copy(part, part, done))
        return fetched[-1:]

    def settle(copies):
        for copy in copies:
            copy.wait()

    q_rows, q_cols = q.shape[:2]
    e_rows, s_rows, t_rows = e.shape[0], s.shape[0], t.shape[0]
    e_cols, s_cols, t_cols = e.shape[1], s.shape[1], t.shape[1]
    got_t = [fetch(t, t_in.at[1 : t_rows + 1])] + fetch_flat(first_w.at[3], w_t)
    got_s = [fetch(s, s_in.at[1 : s_rows + 1])] + fetch_flat(first_w.at[2], w_s)
    got_q = fetch_flat(first_w.at[0], w_q) + [fetch(q, q_in.at[1 : q_rows + 1])]
    got_e = fetch_flat(first_w.at[1], w_e) + [fetch(e, e_in.at[1 : e_rows + 1])]
    got_b_q = fetch_both(first_w.at[0], b_q)
    got_b_t = fetch_both(first_w.at[3], b_t)
    got_b_s = fetch_both(first_w.at[2], b_s)
    got_small = [
        fetch(class_w_in, class_w),
        fetch(bias_in, bias),
        fetch(gain_in, gain),
        fetch(shift_in, shift),
        fetch(labels_in, labels),
    ]
    got_i = [
        fetch_flat(inner_w.at[i], w_i.at[i]) + fetch_both(inner_w.at[i], b_i.at[i]) for i in range(3)
    ]
    got_b_e = fetch_both(first_w.at[1], b_e)

    def exists(offset):
        return me + offset < size if offset > 0 else me + offset >= 0

    def neighbour(offset):
        return {"rows": lax.rem(me + offset + size, size)}

    def edges(lower, upper, before, after, number):
        return [
            (
                pltpu.make_async_remote_copy(
                    src_ref=source,
                    dst_ref=target,
                    send_sem=edge_send.at[number + place],
                    recv_sem=edge_recv.at[number + place],
                    device_id=neighbour(offset),
                    device_id_type=MESH,
                ),
                offset,
            )
            for place, (source, target, offset) in enumerate([(lower, before, 1), (upper, after, -1)])
        ]

    def send(pairs):
        for copy, offset in pairs:
            pl.when(exists(offset))(copy.start)

    def arrive(pairs):
        for copy, offset in pairs:
            pl.when(exists(-offset))(copy.wait_recv)

    def leave(pairs):
        for copy, offset in pairs:
            pl.when(exists(offset))(copy.wait_send)

    def band_edges(field, number):
        last = field.shape[0] - 1
        return edges(field.at[last - 1], field.at[1], field.at[0], field.at[last], number)

    def line_edges(leaving, landing, number):
        return edges(leaving.at[1], leaving.at[0], landing.at[0], landing.at[1], number)

    t_edges, s_edges = line_edges(t_lent, t_owed, 0), line_edges(s_lent, s_owed, 2)
    t_y_edges, s_y_edges = line_edges(t_leave, t_land, 4), line_edges(s_leave, s_land, 6)
    t_y2_edges, t_y3_edges = line_edges(t_leave2, t_land2, 8), line_edges(t_leave3, t_land3, 20)
    coarse_edges = band_edges(coarse, 10)

    def part_edges(leaving, landing, number, chunks):
        step = leaving.shape[1] // chunks
        return [
            edges(
                leaving.at[1, part], leaving.at[0, part], landing.at[0, part], landing.at[1, part], number
            )
            for part in (pl.ds(k * step, step) for k in range(chunks))
        ]

    e_edges, q_edges = line_edges(e_lent, e_owed, 12), line_edges(q_lent, q_owed, 14)
    coarse_base = line_edges(base_leave.at[0], base_land.at[0], 16)
    fine_base = line_edges(base_leave.at[1], base_land.at[1], 18)
    chunks = part_edges(e_lent, e_owed, 12, E_CHUNKS) + part_edges(q_lent, q_owed, 14, Q_CHUNKS)
    waiting, ticks = list(chunks), list(TICKS)

    def tick():
        for _ in range(ticks.pop(0)):
            send(waiting.pop(0))

    for both in (b_q, b_e, b_s, b_t, *[b_i.at[i] for i in range(3)]):
        depth = both.shape[0] // 4
        for row, column in ((3 * depth, 0), (0, width)):
            both[row : row + depth, column : column + width] = jnp.zeros((depth, width), BF16)

    for field in (q_in, e_in, s_in, t_in):
        for row in (0, field.shape[0] - 1):
            field[row] = jnp.zeros(field.shape[1:], BF16)

    up_t[...] = doubling(*up_t.shape, 1)
    up_s[...] = doubling(*up_s.shape, 1)

    def lend(x_ref, flat_ref, lent, kind, place):
        depth, last = x_ref.shape[2], x_ref.shape[0] - 2
        for side, row, down in ((0, 1, 2), (1, last, 0)):
            term = border_term(x_ref[row], flat_ref[down * depth : (down + 1) * depth])
            base = jnp.sum(term, axis=0, keepdims=True) / term.shape[0]
            lent[side] = (term - base).astype(BF16)
            base_leave[kind, side, place : place + 1] = base

    phase("lend_t")
    settle(got_t)
    lend(t_in, w_t, t_lent, 0, 0)
    phase("lend_s")
    settle(got_s)
    lend(s_in, w_s, s_lent, 0, 1)
    phase("lend_q")
    settle(got_q)
    lend(q_in, w_q, q_lent, 1, 0)
    phase("barrier")
    pl.semaphore_wait(barrier, total - 1)
    send(t_edges)
    send(coarse_base)
    send(s_edges)
    phase("lend_e")
    settle(got_e)
    lend(e_in, w_e, e_lent, 1, 1)
    send(fine_base)
    tick()

    def slab_copy(number, distance, sender):
        return pltpu.make_async_remote_copy(
            src_ref=slab.at[number],
            dst_ref=slabs.at[number, sender],
            send_sem=slab_send.at[number],
            recv_sem=slab_recv.at[number],
            device_id=neighbour(distance),
            device_id_type=MESH,
        )

    def slab_all(number):
        rest = slabs.at[number, 0 : size - 1]
        return pltpu.make_async_remote_copy(
            src_ref=rest,
            dst_ref=rest,
            send_sem=slab_send.at[number],
            recv_sem=slab_recv.at[number],
            device_id=neighbour(1),
            device_id_type=MESH,
        )

    def announce(number, stat, cols):
        rows = stat.shape[0]
        sums = stat[:, 0:1]
        channel = jnp.sum(sums, axis=0)
        mean = group_fold(channel) / (rows * cols * (width // GROUPS))
        strays = sums / cols - mean
        slab[number, 0:1] = channel
        slab[number, 1:2] = jnp.sum(stat[:, 1:2] + cols * (strays * strays), axis=0)
        for distance in range(1, size):
            slab_copy(number, distance, me).start()
        slabs[number, me] = slab[number]

    def gather(number, rows, cols):
        slab_all(number).wait_recv()
        count = rows * cols * (width // GROUPS)
        every = slabs[number].reshape(2 * size, width)
        every = group_fold(every).reshape(size, 2, width)
        means = every[:, 0:1] / count
        mean = jnp.sum(means, axis=0) / size
        strays = means - mean
        squares = jnp.sum(every[:, 1:2] + count * (strays * strays), axis=0)
        return mean, squares / (count * size)

    def activation(stat, layer):
        mean, var = stat
        factor = gain[layer : layer + 1] * lax.rsqrt(var + NORM_FLOOR)
        offset = shift[layer : layer + 1]
        return lambda y: jnp.maximum((y - mean) * factor + offset, 0.0).astype(BF16)

    def part_with(field, leaving, number, pairs):
        own = field.shape[0] - 2
        mean = slab[number, 0:1] / (own * field.shape[1])
        leaving[0] = (field[1] - mean).astype(BF16)
        leaving[1] = (field[own] - mean).astype(BF16)
        send(pairs)

    def frame(field, landing, number, pairs):
        own = field.shape[0] - 2
        arrive(pairs)

        def accept(place, row, sender):
            mean = slabs[number, sender, 0:1] / (own * field.shape[1])
            field[row] = landing[place].astype(F32) + mean

        pl.when(me > 0)(lambda: accept(0, 0, lax.rem(me - 1 + size, size)))
        pl.when(me < size - 1)(lambda: accept(1, own + 1, lax.rem(me + 1, size)))

        @pl.when(me == 0)
        def _():
            field[0] = field[1]

        @pl.when(me == size - 1)
        def _():
            field[own + 1] = field[own]

    def grow(field, grown, up, act):
        own = field.shape[0] - 2
        lines = jnp.concatenate([act(field[row]) for row in range(own + 2)], axis=1)
        lines = jnp.dot(up[...], lines, preferred_element_type=F32)
        for row in range(own + 1):
            here = lines[:, row * width : (row + 1) * width]
            below = lines[:, (row + 1) * width : (row + 2) * width]
            grown[2 * row] = (0.75 * here + 0.25 * below).astype(BF16)
            grown[2 * row + 1] = (0.25 * here + 0.75 * below).astype(BF16)

        @pl.when(me == 0)
        def _():
            grown[0] = jnp.zeros(grown.shape[1:], BF16)

        @pl.when(me == size - 1)
        def _():
            grown[2 * own + 1] = jnp.zeros(grown.shape[1:], BF16)

    def convolve(x_ref, weights, y_ref, stat_ref, offset):
        count, cols = x_ref.shape[0] - 2, x_ref.shape[1]
        pairs = max(
            r for r in range(1, count // 2 + 1) if count % (2 * r) == 0 and (r == 1 or r * cols <= 512)
        )
        for index in range(count // (2 * pairs)):
            conv_to(x_ref, weights, y_ref, stat_ref, 2 * pairs * index, pairs, offset)

    done, pairs_left = [0], list(PAIRS)

    def q_blocks():
        first, last = done[0], done[0] + pairs_left.pop(0)
        done[0] = last = last if pairs_left else q_rows // 2

        for index in range(first, last):
            conv_to(q_in, (w_q, b_q), q_y, q_stat, 2 * index, 1, 0)
            tick()

    def mend(y_ref, stat_ref, owed, kind, place, pairs, offset):
        arrive(pairs)

        def add(side, row):
            term = owed[side].astype(F32) + base_land[kind, side, place : place + 1]
            keep(y_ref[row + offset] + term, y_ref, stat_ref, row, offset)

        pl.when(me > 0)(lambda: add(0, 0))
        pl.when(me < size - 1)(lambda: add(1, stat_ref.shape[0] - 1))

    phase("q_blocks_a")
    settle(got_b_q)
    q_blocks()
    phase("conv_t")
    settle(got_b_t)
    convolve(t_in, (w_t, b_t), t_y, t_stat, 1)
    phase("mend_t")
    arrive(coarse_base)
    mend(t_y, t_stat, t_owed, 0, 0, t_edges, 1)
    phase("announce_t")
    announce(0, t_stat, t_cols)
    part_with(t_y, t_leave, 0, t_y_edges)
    phase("conv_s")
    settle(got_b_s)
    convolve(s_in, (w_s, b_s), s_y, s_stat, 1)
    phase("mend_s")
    mend(s_y, s_stat, s_owed, 0, 1, s_edges, 1)
    announce(1, s_stat, s_cols)
    part_with(s_y, s_leave, 1, s_y_edges)
    settle(got_small)
    tick()
    phase("q_blocks_b")
    q_blocks()
    phase("gather_t")
    norm = gather(0, t_rows, t_cols)
    settle(got_i[1])
    phase("frame_t")
    frame(t_y, t_land, 0, t_y_edges)
    phase("grow_t")
    grow(t_y, t_grown, up_t, activation(norm, 3))
    phase("conv_t2")
    convolve(t_grown, (w_i.at[1], b_i.at[1]), t_y2, t_stat2, 1)
    phase("announce_t2")
    announce(2, t_stat2, 2 * t_cols)
    part_with(t_y2, t_leave2, 2, t_y2_edges)
    tick()
    phase("conv_e")
    settle(got_b_e)
    convolve(e_in, (w_e, b_e), e_y, e_stat, 0)
    phase("mend_e")
    arrive(fine_base)
    mend(e_y, e_stat, e_owed, 1, 1, e_edges, 0)
    announce(5, e_stat, e_cols)
    tick()
    phase("q_blocks_c")
    q_blocks()
    phase("gather_s")
    norm = gather(1, s_rows, s_cols)
    settle(got_i[0])
    phase("frame_s")
    frame(s_y, s_land, 1, s_y_edges)
    phase("grow_s")
    grow(s_y, s_grown, up_s, activation(norm, 2))
    phase("conv_s2")
    convolve(s_grown, (w_i.at[0], b_i.at[0]), s_y2, s_stat2, 0)
    announce(3, s_stat2, 2 * s_cols)
    tick()
    phase("gather_t2")
    norm = gather(2, 2 * t_rows, 2 * t_cols)
    settle(got_i[2])
    phase("frame_t2")
    frame(t_y2, t_land2, 2, t_y2_edges)
    phase("grow_t2")
    grow(t_y2, t_grown2, up_s, activation(norm, 5))
    phase("conv_t3")
    convolve(t_grown2, (w_i.at[2], b_i.at[2]), t_y3, t_stat3, 1)
    phase("announce_t3")
    announce(4, t_stat3, 4 * t_cols)
    part_with(t_y3, t_leave3, 4, t_y3_edges)
    phase("mend_q")
    mend(q_y, q_stat, q_owed, 1, 0, q_edges, 0)
    announce(6, q_stat, q_cols)
    phase("gather_se")
    s_act = activation(gather(3, 2 * s_rows, 2 * s_cols), 4)
    e_act = activation(gather(5, e_rows, e_cols), 1)
    phase("project")
    class_f[...] = jnp.zeros(class_f.shape, F32)
    class_f[0:classes] = class_w[...].astype(F32)
    class_pad[...] = class_f[...].astype(BF16)
    padded = class_f.shape[0]
    weight = class_pad[...]
    weights = jnp.concatenate([weight] * 2, axis=1)
    across = (((1,), (1,)), ((), ()))

    def project(row, carry):
        lines = jnp.concatenate([e_act(e_y[row]), s_act(s_y2[row])], axis=1)
        coarse[row + 1] = lax.dot_general(weights, lines, across, preferred_element_type=F32)
        return carry

    lax.fori_loop(0, e_rows, project, 0, unroll=4)
    send(coarse_edges)

    phase("gather_q")
    q_act = activation(gather(6, q_rows, q_cols), 0)
    spot = lax.broadcasted_iota(jnp.int32, (padded, classes), 0)
    lane = lax.broadcasted_iota(jnp.int32, (padded, classes), 1)
    bias_col = jnp.sum(jnp.where(spot == lane, bias[...], 0.0), axis=1, keepdims=True)
    phase("score_q")

    def score(row, carry):
        scores[row] = (
            lax.dot_general(weight, q_act(q_y[row]), across, preferred_element_type=F32) + bias_col
        )
        return carry

    lax.fori_loop(0, q_rows, score, 0, unroll=4)
    phase("wait_coarse")
    up_cols = doubling(e_cols, q_cols, 0)
    arrive(coarse_edges)
    leave(coarse_edges)

    @pl.when(me == 0)
    def _():
        coarse[0] = coarse[1]

    @pl.when(me == size - 1)
    def _():
        coarse[e_rows + 1] = coarse[e_rows]

    phase("gather_t3")
    t_act = activation(gather(4, 4 * t_rows, 4 * t_cols), 6)
    phase("frame_t3")
    frame(t_y3, t_land3, 4, t_y3_edges)
    phase("project_t")

    def project_t(row, carry):
        coarse[row] += lax.dot_general(
            weight, t_act(t_y3[row]), across, preferred_element_type=F32
        )
        return carry

    lax.fori_loop(0, e_rows + 2, project_t, 0, unroll=True)
    phase("widen")
    lines = coarse[...].reshape((e_rows + 2) * padded, e_cols)
    high = lines.astype(BF16)
    low = (lines - high.astype(F32)).astype(BF16)
    lines = jnp.dot(high, up_cols, preferred_element_type=F32) + jnp.dot(
        low, up_cols, preferred_element_type=F32
    )
    wide[...] = lines.reshape(wide.shape)
    phase("finish")
    kind = lax.broadcasted_iota(jnp.int32, (padded, q_cols), 0)

    def finish(row, grown):
        line = scores[row] + grown
        scores[row] = line
        powers = jnp.where(kind < classes, jnp.exp(line), 0.0)
        log_total = jnp.log(jnp.sum(powers, axis=0, keepdims=True))
        label = labels[pl.ds(row, 1), :]
        picked = jnp.sum(jnp.where(kind == label, line, 0.0), axis=0, keepdims=True)
        usable = label != IGNORED
        return jnp.where(usable, log_total - picked, 0.0), usable.astype(F32)

    def pair(index, carry):
        here = wide[index + 1]
        upper = finish(2 * index, 0.25 * wide[index] + 0.75 * here)
        lower = finish(2 * index + 1, 0.75 * here + 0.25 * wide[index + 2])
        return carry[0] + upper[0] + lower[0], carry[1] + upper[1] + lower[1]

    zero = jnp.zeros((1, q_cols), F32)
    sums = lax.fori_loop(0, e_rows, pair, (zero, zero), unroll=2)
    phase("loss_send")
    for place, line in enumerate(sums):
        loss_slab[place : place + 1] = sum(
            line[:, k * width : (k + 1) * width] for k in range(q_cols // width)
        )

    def loss_copy(source, target, peer):
        return pltpu.make_async_remote_copy(
            src_ref=source,
            dst_ref=target,
            send_sem=loss_send.at[0],
            recv_sem=loss_recv.at[0],
            device_id=peer,
            device_id_type=MESH,
        )

    for peer in reversed(peers):
        loss_copy(loss_slab, loss_slabs.at[flat], peer).start()
    rest = loss_slabs.at[0 : total - 1]
    loss_all = loss_copy(rest, rest, peers[0])
    loss_slabs[flat] = loss_slab[...]
    phase("output")
    for first in range(0, classes, 8):
        lines = jnp.transpose(scores[:, first : first + 8], (1, 0, 2)).astype(BF16)
        out[first : min(first + 8, classes)] = lines[: min(8, classes - first)]
    phase("leave")
    for pairs in (
        t_edges, s_edges, t_y_edges, s_y_edges, t_y2_edges, t_y3_edges, e_edges, q_edges, coarse_base, fine_base,
    ):
        leave(pairs)
    for number in range(slab.shape[0]):
        slab_all(number).wait_send()
    phase("loss_wait")
    loss_all.wait_recv()
    phase("loss_end")
    ends = jnp.sum(jnp.sum(loss_slabs[...], axis=0), axis=1, keepdims=True)
    loss_out[...] = jnp.broadcast_to(ends[0:1] / jnp.maximum(ends[1:2], 1.0), loss_out.shape)
    loss_all.wait_send()
    phase("")


def make_per_device(shape):
    def per_device(
        feat_quarter,
        feat_eighth,
        feat_sixteenth,
        feat_thirty,
        labels,
        first_weights,
        inner_weights,
        norm_gain,
        norm_shift,
        class_weight,
        class_bias,
    ):
        q, e, s, t = feat_quarter[0], feat_eighth[0], feat_sixteenth[0], feat_thirty[0]
        size = shape["rows"]
        total = size * shape["batch"]
        depth, width = first_weights.shape[3:]
        classes = class_weight.shape[1]
        padded = -(-classes // 8) * 8
        (q_rows, q_cols), (e_rows, e_cols) = q.shape[:2], e.shape[:2]
        (s_rows, s_cols), (t_rows, t_cols) = s.shape[:2], t.shape[:2]

        def framed(rows, cols, channels, kind=BF16):
            return pltpu.VMEM((rows + 2, cols, channels), kind)

        def field(rows, cols):
            return pltpu.VMEM((rows, cols, width), F32)

        def stat(rows):
            return pltpu.VMEM((rows, 8, width), F32)

        def line(cols):
            return pltpu.VMEM((2, cols, width), BF16)

        small = [labels[0], norm_gain, norm_shift, class_weight.T, class_bias[None]]
        scratch = [
            *[pltpu.VMEM(x.shape, x.dtype) for x in small],
            framed(q_rows, q_cols, depth),
            framed(e_rows, e_cols, depth),
            framed(s_rows, s_cols, depth),
            framed(t_rows, t_cols, depth),
            *[pltpu.VMEM((3 * depth, 3 * width), BF16)] * 4,
            pltpu.VMEM((3, 3 * width, 3 * width), BF16),
            *[pltpu.VMEM((4 * depth, 2 * width), BF16)] * 4,
            pltpu.VMEM((3, 4 * width, 2 * width), BF16),
            field(q_rows, q_cols),
            field(e_rows, e_cols),
            framed(s_rows, s_cols, width, F32),
            framed(t_rows, t_cols, width, F32),
            framed(2 * s_rows, 2 * s_cols, width),
            field(2 * s_rows, 2 * s_cols),
            framed(2 * t_rows, 2 * t_cols, width),
            framed(2 * t_rows, 2 * t_cols, width, F32),
            framed(4 * t_rows, 4 * t_cols, width),
            framed(4 * t_rows, 4 * t_cols, width, F32),
            *[
                line(c)
                for c in (t_cols, s_cols, 2 * t_cols, 4 * t_cols, t_cols, s_cols, e_cols, q_cols)
            ]
            * 2,
            *[pltpu.VMEM((2, 2, 2, width), F32)] * 2,
            stat(q_rows),
            stat(e_rows),
            stat(s_rows),
            stat(t_rows),
            stat(2 * s_rows),
            stat(2 * t_rows),
            stat(4 * t_rows),
            pltpu.VMEM((7, 2, width), F32),
            pltpu.VMEM((7, size, 2, width), F32),
            pltpu.VMEM((padded, width), F32),
            pltpu.VMEM((padded, width), BF16),
            pltpu.VMEM((2 * t_cols, t_cols), BF16),
            pltpu.VMEM((2 * s_cols, s_cols), BF16),
            framed(e_rows, padded, e_cols, F32),
            framed(e_rows, padded, q_cols, F32),
            pltpu.VMEM((q_rows, padded, q_cols), F32),
            pltpu.VMEM((2, width), F32),
            pltpu.VMEM((total, 2, width), F32),
            *[pltpu.SemaphoreType.DMA((count,)) for count in (32, 22, 22, 7, 7, 1, 1)],
        ]
        away, held = pl.BlockSpec(memory_space=pl.ANY), pl.BlockSpec(memory_space=pltpu.VMEM)
        operands = (q, e, s, t, small[0], first_weights, inner_weights, *small[1:])
        logits, loss = pl.pallas_call(
            functools.partial(head_kernel, shape),
            out_shape=(
                jax.ShapeDtypeStruct((classes, q_rows, q_cols), BF16),
                jax.ShapeDtypeStruct((8, width), F32),
            ),
            in_specs=[away] * 11,
            out_specs=(held, held),
            scratch_shapes=scratch,
            compiler_params=pltpu.CompilerParams(
                collective_id=0, has_side_effects=True, vmem_limit_bytes=32 << 20
            ),
        )(*[pltpu.with_memory_space_constraint(x, pltpu.HBM) for x in operands])
        return (logits[None], loss[0, 0])

    return per_device


def solution(mesh):
    in_specs = (
        P("batch", "rows", None, None),
        P("batch", "rows", None, None),
        P("batch", "rows", None, None),
        P("batch", "rows", None, None),
        P("batch", "rows", None),
        P(),
        P(),
        P(),
        P(),
        P(),
        P(),
    )
    out_specs = (P("batch", None, "rows", None), P())
    return jax.shard_map(
        make_per_device(dict(mesh.shape)),
        mesh=mesh,
        in_specs=in_specs,
        out_specs=out_specs,
        check_vma=False,
    )
```

```python
import functools

import jax
import jax.numpy as jnp
from jax import lax
from jax.experimental import pallas as pl
from jax.experimental.pallas import tpu as pltpu
from jax.sharding import PartitionSpec as P

GROUPS = 32
NORM_FLOOR = 0.05
IGNORED = 255
Q_CHUNKS = 4
E_CHUNKS = 2
TICKS = (2, 0, 0, 0, 0, 1, 1, 0, 0, 2, 0, 0, 0)
PAIRS = (4, 1, 3)
MESH = pl.DeviceIdType.MESH
F32 = jnp.float32
BF16 = jnp.bfloat16


def phase(name):
    pass


def group_fold(x):
    width = x.shape[-1]
    lane = lax.broadcasted_iota(jnp.int32, x.shape, x.ndim - 1)
    step = 1
    while step < width // GROUPS:
        ahead = pltpu.roll(x, width - step, x.ndim - 1)
        behind = pltpu.roll(x, step, x.ndim - 1)
        x = x + jnp.where(lax.rem(lane, 2 * step) < step, ahead, behind)
        step *= 2
    return x


def doubling(rows, cols, source_axis):
    source = lax.broadcasted_iota(jnp.int32, (rows, cols), source_axis)
    target = lax.broadcasted_iota(jnp.int32, (rows, cols), 1 - source_axis)
    count = (rows, cols)[source_axis]
    near = lax.div(target, 2)
    far = jnp.clip(near + 2 * lax.rem(target, 2) - 1, 0, count - 1)
    return (
        0.75 * (source == near).astype(F32) + 0.25 * (source == far).astype(F32)
    ).astype(BF16)


def from_left(taps, cols):
    col = lax.rem(lax.broadcasted_iota(jnp.int32, taps.shape, 0), cols)
    return jnp.where(col == 0, 0.0, pltpu.roll(taps, 1, 0))


def from_right(taps, cols):
    count = taps.shape[0]
    col = lax.rem(lax.broadcasted_iota(jnp.int32, taps.shape, 0), cols)
    return jnp.where(col == cols - 1, 0.0, pltpu.roll(taps, count - 1, 0))


def keep(y, y_ref, stat_ref, row, offset):
    y_ref[row + offset] = y
    sums = jnp.sum(y, axis=0, keepdims=True)
    centred = y - sums / y.shape[0]
    stat_ref[row, 0:1] = sums
    stat_ref[row, 1:2] = jnp.sum(centred * centred, axis=0, keepdims=True)


def conv_to(x_ref, weights, y_ref, stat_ref, start, pairs, offset):
    flat, both = weights
    cols, depth = x_ref.shape[1:]
    width = flat.shape[1] // 3
    lines = jnp.concatenate(
        [
            jnp.concatenate([x_ref[start + 2 * k + down] for k in range(pairs)], axis=0)
            for down in range(4)
        ],
        axis=1,
    )
    first = jnp.dot(lines[:, : 3 * depth], flat[:, : 2 * width], preferred_element_type=F32)
    shared = jnp.dot(lines, both[...], preferred_element_type=F32)
    last = jnp.dot(lines[:, depth:], flat[:, width:], preferred_element_type=F32)
    upper = first[:, width:] + from_left(first[:, :width], cols) + from_right(shared[:, :width], cols)
    lower = last[:, :width] + from_left(shared[:, width:], cols) + from_right(last[:, width:], cols)
    for k in range(pairs):
        for row, y in ((0, upper), (1, lower)):
            keep(y[k * cols : (k + 1) * cols], y_ref, stat_ref, start + 2 * k + row, offset)


def border_term(line, flat):
    width = flat.shape[1] // 3
    taps = jnp.dot(line, flat, preferred_element_type=F32)
    cols = line.shape[0]
    return (
        taps[:, width : 2 * width]
        + from_left(taps[:, :width], cols)
        + from_right(taps[:, 2 * width :], cols)
    )


def head_kernel(
    shape,
    q, e, s, t, labels_in, first_w, inner_w, gain_in, shift_in, class_w_in, bias_in,
    out, loss_out,
    labels, gain, shift, class_w, bias,
    q_in, e_in, s_in, t_in, w_q, w_e, w_s, w_t, w_i, b_q, b_e, b_s, b_t, b_i,
    q_y, e_y, s_y, t_y, s_grown, s_y2, t_grown, t_y2, t_grown2, t_y3,
    t_leave, s_leave, t_leave2, t_leave3, t_lent, s_lent, e_lent, q_lent,
    t_land, s_land, t_land2, t_land3, t_owed, s_owed, e_owed, q_owed,
    base_leave, base_land, rim_leave, rim_land,
    q_stat, e_stat, s_stat, t_stat, s_stat2, t_stat2, t_stat3,
    slab, slabs, class_f, class_pad, up_t, up_s, coarse, wide, scores, loss_slab, loss_slabs,
    local_sem, edge_send, edge_recv, slab_send, slab_recv, loss_send, loss_recv,
):
    size, images = shape["rows"], shape["batch"]
    total = size * images
    me, image = lax.axis_index("rows"), lax.axis_index("batch")
    flat = image * size + me
    width = q_y.shape[2]
    classes = class_w.shape[0]

    def wrapped(place, distance, count):
        place = place + distance
        return jnp.where(place >= count, place - count, place)

    peers = [
        {"batch": wrapped(image, across, images), "rows": wrapped(me, along, size)}
        for across in range(images)
        for along in range(size)
        if across or along
    ]

    phase("enter")
    barrier = pltpu.get_barrier_semaphore()
    for peer in peers:
        pl.semaphore_signal(barrier, inc=1, device_id=peer, device_id_type=MESH)

    fetched = []

    def fetch(source, target):
        copy = pltpu.make_async_copy(source, target, local_sem.at[len(fetched)])
        copy.start()
        fetched.append(copy)
        return copy

    def block(ref, down, column):
        depth = ref.shape[0] // (3 if ref.shape[1] == 3 * width else 4)
        return ref.at[down * depth : (down + 1) * depth, column * width : (column + 1) * width]

    def fetch_flat(source, target):
        done = local_sem.at[len(fetched)]
        for down in range(3):
            for across in range(3):
                place = block(target, down, across)
                pltpu.make_async_copy(source.at[down, across], place, done).start()
        fetched.append(pltpu.make_async_copy(target, target, done))
        return fetched[-1:]

    def fetch_both(source, target):
        done = local_sem.at[len(fetched)]
        for down in range(3):
            pltpu.make_async_copy(source.at[down, 2], block(target, down, 0), done).start()
            pltpu.make_async_copy(source.at[down, 0], block(target, down + 1, 1), done).start()
        part = target.at[0 : 3 * source.shape[2]]
        fetched.append(pltpu.make_async_copy(part, part, done))
        return fetched[-1:]

    def settle(copies):
        for copy in copies:
            copy.wait()

    q_rows, q_cols = q.shape[:2]
    e_rows, s_rows, t_rows = e.shape[0], s.shape[0], t.shape[0]
    e_cols, s_cols, t_cols = e.shape[1], s.shape[1], t.shape[1]
    got_t = [fetch(t, t_in.at[1 : t_rows + 1])] + fetch_flat(first_w.at[3], w_t)
    got_s = [fetch(s, s_in.at[1 : s_rows + 1])] + fetch_flat(first_w.at[2], w_s)
    got_q = fetch_flat(first_w.at[0], w_q) + [fetch(q, q_in.at[1 : q_rows + 1])]
    got_e = fetch_flat(first_w.at[1], w_e) + [fetch(e, e_in.at[1 : e_rows + 1])]
    got_b_q = fetch_both(first_w.at[0], b_q)
    got_b_t = fetch_both(first_w.at[3], b_t)
    got_b_s = fetch_both(first_w.at[2], b_s)
    got_small = [
        fetch(class_w_in, class_w),
        fetch(bias_in, bias),
        fetch(gain_in, gain),
        fetch(shift_in, shift),
        fetch(labels_in, labels),
    ]
    got_i = [
        fetch_flat(inner_w.at[i], w_i.at[i]) + fetch_both(inner_w.at[i], b_i.at[i]) for i in range(3)
    ]
    got_b_e = fetch_both(first_w.at[1], b_e)

    def exists(offset):
        return me + offset < size if offset > 0 else me + offset >= 0

    def neighbour(offset):
        return {"rows": lax.rem(me + offset + size, size)}

    def edges(lower, upper, before, after, number):
        return [
            (
                pltpu.make_async_remote_copy(
                    src_ref=source,
                    dst_ref=target,
                    send_sem=edge_send.at[number + place],
                    recv_sem=edge_recv.at[number + place],
                    device_id=neighbour(offset),
                    device_id_type=MESH,
                ),
                offset,
            )
            for place, (source, target, offset) in enumerate([(lower, before, 1), (upper, after, -1)])
        ]

    def send(pairs):
        for copy, offset in pairs:
            pl.when(exists(offset))(copy.start)

    def arrive(pairs):
        for copy, offset in pairs:
            pl.when(exists(-offset))(copy.wait_recv)

    def leave(pairs):
        for copy, offset in pairs:
            pl.when(exists(offset))(copy.wait_send)

    def band_edges(field, number):
        last = field.shape[0] - 1
        return edges(field.at[last - 1], field.at[1], field.at[0], field.at[last], number)

    def line_edges(leaving, landing, number):
        return edges(leaving.at[1], leaving.at[0], landing.at[0], landing.at[1], number)

    t_edges, s_edges = line_edges(t_lent, t_owed, 0), line_edges(s_lent, s_owed, 2)
    t_y_edges, s_y_edges = line_edges(t_leave, t_land, 4), line_edges(s_leave, s_land, 6)
    t_y2_edges, t_y3_edges = line_edges(t_leave2, t_land2, 8), line_edges(t_leave3, t_land3, 20)
    coarse_edges = line_edges(rim_leave, rim_land, 10)

    def part_edges(leaving, landing, number, chunks):
        step = leaving.shape[1] // chunks
        return [
            edges(
                leaving.at[1, part], leaving.at[0, part], landing.at[0, part], landing.at[1, part], number
            )
            for part in (pl.ds(k * step, step) for k in range(chunks))
        ]

    e_edges, q_edges = line_edges(e_lent, e_owed, 12), line_edges(q_lent, q_owed, 14)
    coarse_base = line_edges(base_leave.at[0], base_land.at[0], 16)
    fine_base = line_edges(base_leave.at[1], base_land.at[1], 18)
    chunks = part_edges(e_lent, e_owed, 12, E_CHUNKS) + part_edges(q_lent, q_owed, 14, Q_CHUNKS)
    waiting, ticks = list(chunks), list(TICKS)

    def tick():
        for _ in range(ticks.pop(0)):
            send(waiting.pop(0))

    for both in (b_q, b_e, b_s, b_t, *[b_i.at[i] for i in range(3)]):
        depth = both.shape[0] // 4
        for row, column in ((3 * depth, 0), (0, width)):
            both[row : row + depth, column : column + width] = jnp.zeros((depth, width), BF16)

    for field in (q_in, e_in, s_in, t_in):
        for row in (0, field.shape[0] - 1):
            field[row] = jnp.zeros(field.shape[1:], BF16)

    up_t[...] = doubling(*up_t.shape, 1)
    up_s[...] = doubling(*up_s.shape, 1)

    def lend(x_ref, flat_ref, lent, kind, place):
        depth, last = x_ref.shape[2], x_ref.shape[0] - 2
        for side, row, down in ((0, 1, 2), (1, last, 0)):
            term = border_term(x_ref[row], flat_ref[down * depth : (down + 1) * depth])
            base = jnp.sum(term, axis=0, keepdims=True) / term.shape[0]
            lent[side] = (term - base).astype(BF16)
            base_leave[kind, side, place : place + 1] = base

    phase("lend_t")
    settle(got_t)
    lend(t_in, w_t, t_lent, 0, 0)
    phase("lend_s")
    settle(got_s)
    lend(s_in, w_s, s_lent, 0, 1)
    phase("lend_q")
    settle(got_q)
    lend(q_in, w_q, q_lent, 1, 0)
    phase("barrier")
    pl.semaphore_wait(barrier, total - 1)
    send(t_edges)
    send(coarse_base)
    send(s_edges)
    phase("lend_e")
    settle(got_e)
    lend(e_in, w_e, e_lent, 1, 1)
    send(fine_base)
    tick()

    def slab_copy(number, distance, sender):
        return pltpu.make_async_remote_copy(
            src_ref=slab.at[number],
            dst_ref=slabs.at[number, sender],
            send_sem=slab_send.at[number],
            recv_sem=slab_recv.at[number],
            device_id=neighbour(distance),
            device_id_type=MESH,
        )

    def slab_all(number):
        rest = slabs.at[number, 0 : size - 1]
        return pltpu.make_async_remote_copy(
            src_ref=rest,
            dst_ref=rest,
            send_sem=slab_send.at[number],
            recv_sem=slab_recv.at[number],
            device_id=neighbour(1),
            device_id_type=MESH,
        )

    def announce(number, stat, cols):
        rows = stat.shape[0]
        sums = stat[:, 0:1]
        channel = jnp.sum(sums, axis=0)
        mean = group_fold(channel) / (rows * cols * (width // GROUPS))
        strays = sums / cols - mean
        slab[number, 0:1] = channel
        slab[number, 1:2] = jnp.sum(stat[:, 1:2] + cols * (strays * strays), axis=0)
        for distance in range(1, size):
            slab_copy(number, distance, me).start()
        slabs[number, me] = slab[number]

    def gather(number, rows, cols):
        slab_all(number).wait_recv()
        count = rows * cols * (width // GROUPS)
        every = slabs[number].reshape(2 * size, width)
        every = group_fold(every).reshape(size, 2, width)
        means = every[:, 0:1] / count
        mean = jnp.sum(means, axis=0) / size
        strays = means - mean
        squares = jnp.sum(every[:, 1:2] + count * (strays * strays), axis=0)
        return mean, squares / (count * size)

    def activation(stat, layer):
        mean, var = stat
        factor = gain[layer : layer + 1] * lax.rsqrt(var + NORM_FLOOR)
        offset = shift[layer : layer + 1]
        return lambda y: jnp.maximum((y - mean) * factor + offset, 0.0).astype(BF16)

    def part_with(field, leaving, number, pairs):
        own = field.shape[0] - 2
        mean = slab[number, 0:1] / (own * field.shape[1])
        leaving[0] = (field[1] - mean).astype(BF16)
        leaving[1] = (field[own] - mean).astype(BF16)
        send(pairs)

    def frame(field, landing, number, pairs):
        own = field.shape[0] - 2
        arrive(pairs)

        def accept(place, row, sender):
            mean = slabs[number, sender, 0:1] / (own * field.shape[1])
            field[row] = landing[place].astype(F32) + mean

        pl.when(me > 0)(lambda: accept(0, 0, lax.rem(me - 1 + size, size)))
        pl.when(me < size - 1)(lambda: accept(1, own + 1, lax.rem(me + 1, size)))

        @pl.when(me == 0)
        def _():
            field[0] = field[1]

        @pl.when(me == size - 1)
        def _():
            field[own + 1] = field[own]

    def grow(field, grown, up, act):
        own = field.shape[0] - 2
        lines = jnp.concatenate([act(field[row]) for row in range(own + 2)], axis=1)
        lines = jnp.dot(up[...], lines, preferred_element_type=F32)
        for row in range(own + 1):
            here = lines[:, row * width : (row + 1) * width]
            below = lines[:, (row + 1) * width : (row + 2) * width]
            grown[2 * row] = (0.75 * here + 0.25 * below).astype(BF16)
            grown[2 * row + 1] = (0.25 * here + 0.75 * below).astype(BF16)

        @pl.when(me == 0)
        def _():
            grown[0] = jnp.zeros(grown.shape[1:], BF16)

        @pl.when(me == size - 1)
        def _():
            grown[2 * own + 1] = jnp.zeros(grown.shape[1:], BF16)

    def convolve(x_ref, weights, y_ref, stat_ref, offset):
        count, cols = x_ref.shape[0] - 2, x_ref.shape[1]
        pairs = max(
            r for r in range(1, count // 2 + 1) if count % (2 * r) == 0 and (r == 1 or r * cols <= 512)
        )
        for index in range(count // (2 * pairs)):
            conv_to(x_ref, weights, y_ref, stat_ref, 2 * pairs * index, pairs, offset)

    done, pairs_left = [0], list(PAIRS)

    def q_blocks():
        first, last = done[0], done[0] + pairs_left.pop(0)
        done[0] = last = last if pairs_left else q_rows // 2

        for index in range(first, last):
            conv_to(q_in, (w_q, b_q), q_y, q_stat, 2 * index, 1, 0)
            tick()

    def mend(y_ref, stat_ref, owed, kind, place, pairs, offset):
        arrive(pairs)

        def add(side, row):
            term = owed[side].astype(F32) + base_land[kind, side, place : place + 1]
            keep(y_ref[row + offset] + term, y_ref, stat_ref, row, offset)

        pl.when(me > 0)(lambda: add(0, 0))
        pl.when(me < size - 1)(lambda: add(1, stat_ref.shape[0] - 1))

    phase("q_blocks_a")
    settle(got_b_q)
    q_blocks()
    phase("conv_t")
    settle(got_b_t)
    convolve(t_in, (w_t, b_t), t_y, t_stat, 1)
    phase("mend_t")
    arrive(coarse_base)
    mend(t_y, t_stat, t_owed, 0, 0, t_edges, 1)
    phase("announce_t")
    announce(0, t_stat, t_cols)
    part_with(t_y, t_leave, 0, t_y_edges)
    phase("conv_s")
    settle(got_b_s)
    convolve(s_in, (w_s, b_s), s_y, s_stat, 1)
    phase("mend_s")
    mend(s_y, s_stat, s_owed, 0, 1, s_edges, 1)
    announce(1, s_stat, s_cols)
    part_with(s_y, s_leave, 1, s_y_edges)
    settle(got_small)
    tick()
    phase("conv_e")
    settle(got_b_e)
    convolve(e_in, (w_e, b_e), e_y, e_stat, 0)
    phase("mend_e")
    arrive(fine_base)
    mend(e_y, e_stat, e_owed, 1, 1, e_edges, 0)
    announce(5, e_stat, e_cols)
    tick()
    phase("q_blocks_b")
    q_blocks()
    phase("gather_t")
    norm = gather(0, t_rows, t_cols)
    settle(got_i[1])
    phase("frame_t")
    frame(t_y, t_land, 0, t_y_edges)
    phase("grow_t")
    grow(t_y, t_grown, up_t, activation(norm, 3))
    phase("conv_t2")
    convolve(t_grown, (w_i.at[1], b_i.at[1]), t_y2, t_stat2, 1)
    phase("announce_t2")
    announce(2, t_stat2, 2 * t_cols)
    part_with(t_y2, t_leave2, 2, t_y2_edges)
    tick()
    phase("gather_s")
    norm = gather(1, s_rows, s_cols)
    settle(got_i[0])
    phase("frame_s")
    frame(s_y, s_land, 1, s_y_edges)
    phase("grow_s")
    grow(s_y, s_grown, up_s, activation(norm, 2))
    phase("conv_s2")
    convolve(s_grown, (w_i.at[0], b_i.at[0]), s_y2, s_stat2, 0)
    announce(3, s_stat2, 2 * s_cols)
    tick()
    phase("q_blocks_c")
    q_blocks()
    phase("gather_t2")
    norm = gather(2, 2 * t_rows, 2 * t_cols)
    settle(got_i[2])
    phase("frame_t2")
    frame(t_y2, t_land2, 2, t_y2_edges)
    phase("grow_t2")
    grow(t_y2, t_grown2, up_s, activation(norm, 5))
    phase("conv_t3")
    convolve(t_grown2, (w_i.at[2], b_i.at[2]), t_y3, t_stat3, 1)
    phase("announce_t3")
    announce(4, t_stat3, 4 * t_cols)
    part_with(t_y3, t_leave3, 4, t_y3_edges)
    phase("mend_q")
    mend(q_y, q_stat, q_owed, 1, 0, q_edges, 0)
    announce(6, q_stat, q_cols)
    phase("gather_se")
    s_act = activation(gather(3, 2 * s_rows, 2 * s_cols), 4)
    e_act = activation(gather(5, e_rows, e_cols), 1)
    phase("project")
    class_f[...] = jnp.zeros(class_f.shape, F32)
    class_f[0:classes] = class_w[...].astype(F32)
    class_pad[...] = class_f[...].astype(BF16)
    padded = class_f.shape[0]
    weight = class_pad[...]
    weights = jnp.concatenate([weight] * 2, axis=1)
    across = (((1,), (1,)), ((), ()))

    def project(row, carry):
        lines = jnp.concatenate([e_act(e_y[row]), s_act(s_y2[row])], axis=1)
        coarse[row + 1] = lax.dot_general(weights, lines, across, preferred_element_type=F32)
        return carry

    lax.fori_loop(0, e_rows, project, 0, unroll=4)
    rim_leave[0] = coarse[1].astype(BF16)
    rim_leave[1] = coarse[e_rows].astype(BF16)
    send(coarse_edges)
    coarse[0] = jnp.zeros(coarse.shape[1:], F32)
    coarse[e_rows + 1] = jnp.zeros(coarse.shape[1:], F32)
    up_cols = doubling(e_cols, q_cols, 0)

    phase("gather_t3")
    t_act = activation(gather(4, 4 * t_rows, 4 * t_cols), 6)
    phase("frame_t3")
    frame(t_y3, t_land3, 4, t_y3_edges)
    phase("project_t")

    def project_t(row, carry):
        coarse[row] += lax.dot_general(
            weight, t_act(t_y3[row]), across, preferred_element_type=F32
        )
        return carry

    lax.fori_loop(0, e_rows + 2, project_t, 0, unroll=True)
    phase("wait_coarse")
    arrive(coarse_edges)
    for beyond, row, own, side in ((me == 0, 0, 1, 0), (me == size - 1, e_rows + 1, e_rows, 1)):

        @pl.when(beyond)
        def _():
            coarse[row] = coarse[own]

        @pl.when(jnp.logical_not(beyond))
        def _():
            coarse[row] += rim_land[side].astype(F32)

    phase("widen")
    lines = coarse[...].reshape((e_rows + 2) * padded, e_cols)
    high = lines.astype(BF16)
    low = (lines - high.astype(F32)).astype(BF16)
    lines = jnp.dot(high, up_cols, preferred_element_type=F32) + jnp.dot(
        low, up_cols, preferred_element_type=F32
    )
    wide[...] = lines.reshape(wide.shape)
    phase("gather_q")
    spot = lax.broadcasted_iota(jnp.int32, (padded, classes), 0)
    lane = lax.broadcasted_iota(jnp.int32, (padded, classes), 1)
    bias_col = jnp.sum(jnp.where(spot == lane, bias[...], 0.0), axis=1, keepdims=True)
    q_act = activation(gather(6, q_rows, q_cols), 0)
    phase("finish")
    kind = lax.broadcasted_iota(jnp.int32, (padded, q_cols), 0)

    def finish(row, grown):
        line = lax.dot_general(weight, q_act(q_y[row]), across, preferred_element_type=F32)
        line = line + bias_col + grown
        scores[row] = line
        powers = jnp.where(kind < classes, jnp.exp(line), 0.0)
        log_total = jnp.log(jnp.sum(powers, axis=0, keepdims=True))
        label = labels[pl.ds(row, 1), :]
        picked = jnp.sum(jnp.where(kind == label, line, 0.0), axis=0, keepdims=True)
        usable = label != IGNORED
        return jnp.where(usable, log_total - picked, 0.0), usable.astype(F32)

    def pair(index, carry):
        here = wide[index + 1]
        upper = finish(2 * index, 0.25 * wide[index] + 0.75 * here)
        lower = finish(2 * index + 1, 0.75 * here + 0.25 * wide[index + 2])
        return carry[0] + upper[0] + lower[0], carry[1] + upper[1] + lower[1]

    zero = jnp.zeros((1, q_cols), F32)
    sums = lax.fori_loop(0, e_rows, pair, (zero, zero), unroll=4)
    phase("loss_send")
    for place, line in enumerate(sums):
        loss_slab[place : place + 1] = sum(
            line[:, k * width : (k + 1) * width] for k in range(q_cols // width)
        )

    def loss_copy(source, target, peer):
        return pltpu.make_async_remote_copy(
            src_ref=source,
            dst_ref=target,
            send_sem=loss_send.at[0],
            recv_sem=loss_recv.at[0],
            device_id=peer,
            device_id_type=MESH,
        )

    for peer in reversed(peers):
        loss_copy(loss_slab, loss_slabs.at[flat], peer).start()
    rest = loss_slabs.at[0 : total - 1]
    loss_all = loss_copy(rest, rest, peers[0])
    loss_slabs[flat] = loss_slab[...]
    phase("output")
    for first in range(0, classes, 8):
        lines = jnp.transpose(scores[:, first : first + 8], (1, 0, 2)).astype(BF16)
        out[first : min(first + 8, classes)] = lines[: min(8, classes - first)]
    phase("leave")
    for pairs in (
        t_edges, s_edges, t_y_edges, s_y_edges, t_y2_edges, t_y3_edges, coarse_edges, e_edges, q_edges, coarse_base, fine_base,
    ):
        leave(pairs)
    for number in range(slab.shape[0]):
        slab_all(number).wait_send()
    phase("loss_wait")
    loss_all.wait_recv()
    phase("loss_end")
    ends = jnp.sum(jnp.sum(loss_slabs[...], axis=0), axis=1, keepdims=True)
    loss_out[...] = jnp.broadcast_to(ends[0:1] / jnp.maximum(ends[1:2], 1.0), loss_out.shape)
    loss_all.wait_send()
    phase("")


def make_per_device(shape):
    def per_device(
        feat_quarter,
        feat_eighth,
        feat_sixteenth,
        feat_thirty,
        labels,
        first_weights,
        inner_weights,
        norm_gain,
        norm_shift,
        class_weight,
        class_bias,
    ):
        q, e, s, t = feat_quarter[0], feat_eighth[0], feat_sixteenth[0], feat_thirty[0]
        size = shape["rows"]
        total = size * shape["batch"]
        depth, width = first_weights.shape[3:]
        classes = class_weight.shape[1]
        padded = -(-classes // 8) * 8
        (q_rows, q_cols), (e_rows, e_cols) = q.shape[:2], e.shape[:2]
        (s_rows, s_cols), (t_rows, t_cols) = s.shape[:2], t.shape[:2]

        def framed(rows, cols, channels, kind=BF16):
            return pltpu.VMEM((rows + 2, cols, channels), kind)

        def field(rows, cols):
            return pltpu.VMEM((rows, cols, width), F32)

        def stat(rows):
            return pltpu.VMEM((rows, 8, width), F32)

        def line(cols):
            return pltpu.VMEM((2, cols, width), BF16)

        small = [labels[0], norm_gain, norm_shift, class_weight.T, class_bias[None]]
        scratch = [
            *[pltpu.VMEM(x.shape, x.dtype) for x in small],
            framed(q_rows, q_cols, depth),
            framed(e_rows, e_cols, depth),
            framed(s_rows, s_cols, depth),
            framed(t_rows, t_cols, depth),
            *[pltpu.VMEM((3 * depth, 3 * width), BF16)] * 4,
            pltpu.VMEM((3, 3 * width, 3 * width), BF16),
            *[pltpu.VMEM((4 * depth, 2 * width), BF16)] * 4,
            pltpu.VMEM((3, 4 * width, 2 * width), BF16),
            field(q_rows, q_cols),
            field(e_rows, e_cols),
            framed(s_rows, s_cols, width, F32),
            framed(t_rows, t_cols, width, F32),
            framed(2 * s_rows, 2 * s_cols, width),
            field(2 * s_rows, 2 * s_cols),
            framed(2 * t_rows, 2 * t_cols, width),
            framed(2 * t_rows, 2 * t_cols, width, F32),
            framed(4 * t_rows, 4 * t_cols, width),
            framed(4 * t_rows, 4 * t_cols, width, F32),
            *[
                line(c)
                for c in (t_cols, s_cols, 2 * t_cols, 4 * t_cols, t_cols, s_cols, e_cols, q_cols)
            ]
            * 2,
            *[pltpu.VMEM((2, 2, 2, width), F32)] * 2,
            *[pltpu.VMEM((2, padded, e_cols), BF16)] * 2,
            stat(q_rows),
            stat(e_rows),
            stat(s_rows),
            stat(t_rows),
            stat(2 * s_rows),
            stat(2 * t_rows),
            stat(4 * t_rows),
            pltpu.VMEM((7, 2, width), F32),
            pltpu.VMEM((7, size, 2, width), F32),
            pltpu.VMEM((padded, width), F32),
            pltpu.VMEM((padded, width), BF16),
            pltpu.VMEM((2 * t_cols, t_cols), BF16),
            pltpu.VMEM((2 * s_cols, s_cols), BF16),
            framed(e_rows, padded, e_cols, F32),
            framed(e_rows, padded, q_cols, F32),
            pltpu.VMEM((q_rows, padded, q_cols), F32),
            pltpu.VMEM((2, width), F32),
            pltpu.VMEM((total, 2, width), F32),
            *[pltpu.SemaphoreType.DMA((count,)) for count in (32, 22, 22, 7, 7, 1, 1)],
        ]
        away, held = pl.BlockSpec(memory_space=pl.ANY), pl.BlockSpec(memory_space=pltpu.VMEM)
        operands = (q, e, s, t, small[0], first_weights, inner_weights, *small[1:])
        logits, loss = pl.pallas_call(
            functools.partial(head_kernel, shape),
            out_shape=(
                jax.ShapeDtypeStruct((classes, q_rows, q_cols), BF16),
                jax.ShapeDtypeStruct((8, width), F32),
            ),
            in_specs=[away] * 11,
            out_specs=(held, held),
            scratch_shapes=scratch,
            compiler_params=pltpu.CompilerParams(
                collective_id=0, has_side_effects=True, vmem_limit_bytes=32 << 20
            ),
        )(*[pltpu.with_memory_space_constraint(x, pltpu.HBM) for x in operands])
        return (logits[None], loss[0, 0])

    return per_device


def solution(mesh):
    in_specs = (
        P("batch", "rows", None, None),
        P("batch", "rows", None, None),
        P("batch", "rows", None, None),
        P("batch", "rows", None, None),
        P("batch", "rows", None),
        P(),
        P(),
        P(),
        P(),
        P(),
        P(),
    )
    out_specs = (P("batch", None, "rows", None), P())
    return jax.shard_map(
        make_per_device(dict(mesh.shape)),
        mesh=mesh,
        in_specs=in_specs,
        out_specs=out_specs,
        check_vma=False,
    )
```

```python
import functools

import jax
import jax.numpy as jnp
from jax import lax
from jax.experimental import pallas as pl
from jax.experimental.pallas import tpu as pltpu
from jax.sharding import PartitionSpec as P

GROUPS = 32
NORM_FLOOR = 0.05
IGNORED = 255
Q_CHUNKS = 4
E_CHUNKS = 2
TICKS = (2, 0, 0, 0, 0, 1, 1, 0, 0, 2, 0, 0, 0)
PAIRS = (4, 1, 3)
MESH = pl.DeviceIdType.MESH
F32 = jnp.float32
BF16 = jnp.bfloat16


def phase(name):
    pass


def group_fold(x):
    width = x.shape[-1]
    lane = lax.broadcasted_iota(jnp.int32, x.shape, x.ndim - 1)
    step = 1
    while step < width // GROUPS:
        ahead = pltpu.roll(x, width - step, x.ndim - 1)
        behind = pltpu.roll(x, step, x.ndim - 1)
        x = x + jnp.where(lax.rem(lane, 2 * step) < step, ahead, behind)
        step *= 2
    return x


def doubling(rows, cols, source_axis):
    source = lax.broadcasted_iota(jnp.int32, (rows, cols), source_axis)
    target = lax.broadcasted_iota(jnp.int32, (rows, cols), 1 - source_axis)
    count = (rows, cols)[source_axis]
    near = lax.div(target, 2)
    far = jnp.clip(near + 2 * lax.rem(target, 2) - 1, 0, count - 1)
    return (
        0.75 * (source == near).astype(F32) + 0.25 * (source == far).astype(F32)
    ).astype(BF16)


def from_left(taps, cols):
    col = lax.rem(lax.broadcasted_iota(jnp.int32, taps.shape, 0), cols)
    return jnp.where(col == 0, 0.0, pltpu.roll(taps, 1, 0))


def from_right(taps, cols):
    count = taps.shape[0]
    col = lax.rem(lax.broadcasted_iota(jnp.int32, taps.shape, 0), cols)
    return jnp.where(col == cols - 1, 0.0, pltpu.roll(taps, count - 1, 0))


def keep(y, y_ref, stat_ref, row, offset):
    y_ref[row + offset] = y
    sums = jnp.sum(y, axis=0, keepdims=True)
    centred = y - sums / y.shape[0]
    stat_ref[row, 0:1] = sums
    stat_ref[row, 1:2] = jnp.sum(centred * centred, axis=0, keepdims=True)


def conv_to(x_ref, weights, y_ref, stat_ref, start, pairs, offset):
    flat, both = weights
    cols, depth = x_ref.shape[1:]
    width = flat.shape[1] // 3
    lines = jnp.concatenate(
        [
            jnp.concatenate([x_ref[start + 2 * k + down] for k in range(pairs)], axis=0)
            for down in range(4)
        ],
        axis=1,
    )
    first = jnp.dot(lines[:, : 3 * depth], flat[:, : 2 * width], preferred_element_type=F32)
    shared = jnp.dot(lines, both[...], preferred_element_type=F32)
    last = jnp.dot(lines[:, depth:], flat[:, width:], preferred_element_type=F32)
    upper = first[:, width:] + from_left(first[:, :width], cols) + from_right(shared[:, :width], cols)
    lower = last[:, :width] + from_left(shared[:, width:], cols) + from_right(last[:, width:], cols)
    for k in range(pairs):
        for row, y in ((0, upper), (1, lower)):
            keep(y[k * cols : (k + 1) * cols], y_ref, stat_ref, start + 2 * k + row, offset)


def border_term(line, flat):
    width = flat.shape[1] // 3
    taps = jnp.dot(line, flat, preferred_element_type=F32)
    cols = line.shape[0]
    return (
        taps[:, width : 2 * width]
        + from_left(taps[:, :width], cols)
        + from_right(taps[:, 2 * width :], cols)
    )


def head_kernel(
    shape,
    q, e, s, t, labels_in, first_w, inner_w, gain_in, shift_in, class_w_in, bias_in,
    out, loss_out,
    labels, gain, shift, class_w, bias,
    q_in, e_in, s_in, t_in, w_q, w_e, w_s, w_t, w_i, b_q, b_e, b_s, b_t, b_i,
    q_y, e_y, s_y, t_y, s_grown, s_y2, t_grown, t_y2, t_grown2, t_y3,
    t_leave, s_leave, t_leave2, t_leave3, t_lent, s_lent, e_lent, q_lent,
    t_land, s_land, t_land2, t_land3, t_owed, s_owed, e_owed, q_owed,
    base_leave, base_land, rim_leave, rim_land,
    q_stat, e_stat, s_stat, t_stat, s_stat2, t_stat2, t_stat3,
    slab, slabs, class_f, class_pad, up_t, up_s, coarse, wide, scores, loss_slab, loss_slabs,
    local_sem, edge_send, edge_recv, slab_send, slab_recv, loss_send, loss_recv,
):
    size, images = shape["rows"], shape["batch"]
    total = size * images
    me, image = lax.axis_index("rows"), lax.axis_index("batch")
    flat = image * size + me
    width = q_y.shape[2]
    classes = class_w.shape[0]

    def wrapped(place, distance, count):
        place = place + distance
        return jnp.where(place >= count, place - count, place)

    peers = [
        {"batch": wrapped(image, across, images), "rows": wrapped(me, along, size)}
        for across in range(images)
        for along in range(size)
        if across or along
    ]

    phase("enter")
    barrier = pltpu.get_barrier_semaphore()
    for peer in peers:
        pl.semaphore_signal(barrier, inc=1, device_id=peer, device_id_type=MESH)

    fetched = []

    def fetch(source, target):
        copy = pltpu.make_async_copy(source, target, local_sem.at[len(fetched)])
        copy.start()
        fetched.append(copy)
        return copy

    def block(ref, down, column):
        depth = ref.shape[0] // (3 if ref.shape[1] == 3 * width else 4)
        return ref.at[down * depth : (down + 1) * depth, column * width : (column + 1) * width]

    def fetch_flat(source, target):
        done = local_sem.at[len(fetched)]
        for down in range(3):
            for across in range(3):
                place = block(target, down, across)
                pltpu.make_async_copy(source.at[down, across], place, done).start()
        fetched.append(pltpu.make_async_copy(target, target, done))
        return fetched[-1:]

    def fetch_both(source, target):
        done = local_sem.at[len(fetched)]
        for down in range(3):
            pltpu.make_async_copy(source.at[down, 2], block(target, down, 0), done).start()
            pltpu.make_async_copy(source.at[down, 0], block(target, down + 1, 1), done).start()
        part = target.at[0 : 3 * source.shape[2]]
        fetched.append(pltpu.make_async_copy(part, part, done))
        return fetched[-1:]

    def settle(copies):
        for copy in copies:
            copy.wait()

    q_rows, q_cols = q.shape[:2]
    e_rows, s_rows, t_rows = e.shape[0], s.shape[0], t.shape[0]
    e_cols, s_cols, t_cols = e.shape[1], s.shape[1], t.shape[1]
    got_t = [fetch(t, t_in.at[1 : t_rows + 1])] + fetch_flat(first_w.at[3], w_t)
    got_s = [fetch(s, s_in.at[1 : s_rows + 1])] + fetch_flat(first_w.at[2], w_s)
    got_q = fetch_flat(first_w.at[0], w_q) + [fetch(q, q_in.at[1 : q_rows + 1])]
    got_e = fetch_flat(first_w.at[1], w_e) + [fetch(e, e_in.at[1 : e_rows + 1])]
    got_b_q = fetch_both(first_w.at[0], b_q)
    got_b_t = fetch_both(first_w.at[3], b_t)
    got_b_s = fetch_both(first_w.at[2], b_s)
    got_small = [
        fetch(class_w_in, class_w),
        fetch(bias_in, bias),
        fetch(gain_in, gain),
        fetch(shift_in, shift),
        fetch(labels_in, labels),
    ]
    got_i = [
        fetch_flat(inner_w.at[i], w_i.at[i]) + fetch_both(inner_w.at[i], b_i.at[i]) for i in range(3)
    ]
    got_b_e = fetch_both(first_w.at[1], b_e)

    def exists(offset):
        return me + offset < size if offset > 0 else me + offset >= 0

    def neighbour(offset):
        return {"rows": lax.rem(me + offset + size, size)}

    def edges(lower, upper, before, after, number):
        return [
            (
                pltpu.make_async_remote_copy(
                    src_ref=source,
                    dst_ref=target,
                    send_sem=edge_send.at[number + place],
                    recv_sem=edge_recv.at[number + place],
                    device_id=neighbour(offset),
                    device_id_type=MESH,
                ),
                offset,
            )
            for place, (source, target, offset) in enumerate([(lower, before, 1), (upper, after, -1)])
        ]

    def send(pairs):
        for copy, offset in pairs:
            pl.when(exists(offset))(copy.start)

    def arrive(pairs):
        for copy, offset in pairs:
            pl.when(exists(-offset))(copy.wait_recv)

    def leave(pairs):
        for copy, offset in pairs:
            pl.when(exists(offset))(copy.wait_send)

    def band_edges(field, number):
        last = field.shape[0] - 1
        return edges(field.at[last - 1], field.at[1], field.at[0], field.at[last], number)

    def line_edges(leaving, landing, number):
        return edges(leaving.at[1], leaving.at[0], landing.at[0], landing.at[1], number)

    t_edges, s_edges = line_edges(t_lent, t_owed, 0), line_edges(s_lent, s_owed, 2)
    t_y_edges, s_y_edges = line_edges(t_leave, t_land, 4), line_edges(s_leave, s_land, 6)
    t_y2_edges, t_y3_edges = line_edges(t_leave2, t_land2, 8), line_edges(t_leave3, t_land3, 20)
    coarse_edges = line_edges(rim_leave, rim_land, 10)

    def part_edges(leaving, landing, number, chunks):
        step = leaving.shape[1] // chunks
        return [
            edges(
                leaving.at[1, part], leaving.at[0, part], landing.at[0, part], landing.at[1, part], number
            )
            for part in (pl.ds(k * step, step) for k in range(chunks))
        ]

    e_edges, q_edges = line_edges(e_lent, e_owed, 12), line_edges(q_lent, q_owed, 14)
    coarse_base = line_edges(base_leave.at[0], base_land.at[0], 16)
    fine_base = line_edges(base_leave.at[1], base_land.at[1], 18)
    chunks = part_edges(e_lent, e_owed, 12, E_CHUNKS) + part_edges(q_lent, q_owed, 14, Q_CHUNKS)
    waiting, ticks = list(chunks), list(TICKS)

    def tick():
        for _ in range(ticks.pop(0)):
            send(waiting.pop(0))

    for both in (b_q, b_e, b_s, b_t, *[b_i.at[i] for i in range(3)]):
        depth = both.shape[0] // 4
        for row, column in ((3 * depth, 0), (0, width)):
            both[row : row + depth, column : column + width] = jnp.zeros((depth, width), BF16)

    for field in (q_in, e_in, s_in, t_in):
        for row in (0, field.shape[0] - 1):
            field[row] = jnp.zeros(field.shape[1:], BF16)

    up_t[...] = doubling(*up_t.shape, 1)
    up_s[...] = doubling(*up_s.shape, 1)

    def lend(x_ref, flat_ref, lent, kind, place):
        depth, last = x_ref.shape[2], x_ref.shape[0] - 2
        for side, row, down in ((0, 1, 2), (1, last, 0)):
            term = border_term(x_ref[row], flat_ref[down * depth : (down + 1) * depth])
            base = jnp.sum(term, axis=0, keepdims=True) / term.shape[0]
            lent[side] = (term - base).astype(BF16)
            base_leave[kind, side, place : place + 1] = base

    phase("lend_t")
    settle(got_t)
    lend(t_in, w_t, t_lent, 0, 0)
    phase("lend_s")
    settle(got_s)
    lend(s_in, w_s, s_lent, 0, 1)
    phase("barrier")
    pl.semaphore_wait(barrier, total - 1)
    send(t_edges)
    send(coarse_base)
    send(s_edges)
    phase("lend_q")
    settle(got_q)
    lend(q_in, w_q, q_lent, 1, 0)
    phase("lend_e")
    settle(got_e)
    lend(e_in, w_e, e_lent, 1, 1)
    send(fine_base)
    tick()

    def slab_copy(number, distance, sender):
        return pltpu.make_async_remote_copy(
            src_ref=slab.at[number],
            dst_ref=slabs.at[number, sender],
            send_sem=slab_send.at[number],
            recv_sem=slab_recv.at[number],
            device_id=neighbour(distance),
            device_id_type=MESH,
        )

    def slab_all(number):
        rest = slabs.at[number, 0 : size - 1]
        return pltpu.make_async_remote_copy(
            src_ref=rest,
            dst_ref=rest,
            send_sem=slab_send.at[number],
            recv_sem=slab_recv.at[number],
            device_id=neighbour(1),
            device_id_type=MESH,
        )

    def announce(number, stat, cols):
        rows = stat.shape[0]
        sums = stat[:, 0:1]
        channel = jnp.sum(sums, axis=0)
        mean = group_fold(channel) / (rows * cols * (width // GROUPS))
        strays = sums / cols - mean
        slab[number, 0:1] = channel
        slab[number, 1:2] = jnp.sum(stat[:, 1:2] + cols * (strays * strays), axis=0)
        for distance in range(1, size):
            slab_copy(number, distance, me).start()
        slabs[number, me] = slab[number]

    def gather(number, rows, cols):
        slab_all(number).wait_recv()
        count = rows * cols * (width // GROUPS)
        every = slabs[number].reshape(2 * size, width)
        every = group_fold(every).reshape(size, 2, width)
        means = every[:, 0:1] / count
        mean = jnp.sum(means, axis=0) / size
        strays = means - mean
        squares = jnp.sum(every[:, 1:2] + count * (strays * strays), axis=0)
        return mean, squares / (count * size)

    def activation(stat, layer):
        mean, var = stat
        factor = gain[layer : layer + 1] * lax.rsqrt(var + NORM_FLOOR)
        offset = shift[layer : layer + 1]
        return lambda y: jnp.maximum((y - mean) * factor + offset, 0.0).astype(BF16)

    def part_with(field, leaving, number, pairs):
        own = field.shape[0] - 2
        mean = slab[number, 0:1] / (own * field.shape[1])
        leaving[0] = (field[1] - mean).astype(BF16)
        leaving[1] = (field[own] - mean).astype(BF16)
        send(pairs)

    def frame(field, landing, number, pairs):
        own = field.shape[0] - 2
        arrive(pairs)

        def accept(place, row, sender):
            mean = slabs[number, sender, 0:1] / (own * field.shape[1])
            field[row] = landing[place].astype(F32) + mean

        pl.when(me > 0)(lambda: accept(0, 0, lax.rem(me - 1 + size, size)))
        pl.when(me < size - 1)(lambda: accept(1, own + 1, lax.rem(me + 1, size)))

        @pl.when(me == 0)
        def _():
            field[0] = field[1]

        @pl.when(me == size - 1)
        def _():
            field[own + 1] = field[own]

    def grow(field, grown, up, act):
        own = field.shape[0] - 2
        lines = jnp.concatenate([act(field[row]) for row in range(own + 2)], axis=1)
        lines = jnp.dot(up[...], lines, preferred_element_type=F32)
        for row in range(own + 1):
            here = lines[:, row * width : (row + 1) * width]
            below = lines[:, (row + 1) * width : (row + 2) * width]
            grown[2 * row] = (0.75 * here + 0.25 * below).astype(BF16)
            grown[2 * row + 1] = (0.25 * here + 0.75 * below).astype(BF16)

        @pl.when(me == 0)
        def _():
            grown[0] = jnp.zeros(grown.shape[1:], BF16)

        @pl.when(me == size - 1)
        def _():
            grown[2 * own + 1] = jnp.zeros(grown.shape[1:], BF16)

    def convolve(x_ref, weights, y_ref, stat_ref, offset):
        count, cols = x_ref.shape[0] - 2, x_ref.shape[1]
        pairs = max(
            r for r in range(1, count // 2 + 1) if count % (2 * r) == 0 and (r == 1 or r * cols <= 512)
        )
        for index in range(count // (2 * pairs)):
            conv_to(x_ref, weights, y_ref, stat_ref, 2 * pairs * index, pairs, offset)

    done, pairs_left = [0], list(PAIRS)

    def q_blocks():
        first, last = done[0], done[0] + pairs_left.pop(0)
        done[0] = last = last if pairs_left else q_rows // 2

        for index in range(first, last):
            conv_to(q_in, (w_q, b_q), q_y, q_stat, 2 * index, 1, 0)
            tick()

    def mend(y_ref, stat_ref, owed, kind, place, pairs, offset):
        arrive(pairs)

        def add(side, row):
            term = owed[side].astype(F32) + base_land[kind, side, place : place + 1]
            keep(y_ref[row + offset] + term, y_ref, stat_ref, row, offset)

        pl.when(me > 0)(lambda: add(0, 0))
        pl.when(me < size - 1)(lambda: add(1, stat_ref.shape[0] - 1))

    phase("q_blocks_a")
    settle(got_b_q)
    q_blocks()
    phase("conv_t")
    settle(got_b_t)
    convolve(t_in, (w_t, b_t), t_y, t_stat, 1)
    phase("mend_t")
    arrive(coarse_base)
    mend(t_y, t_stat, t_owed, 0, 0, t_edges, 1)
    phase("announce_t")
    announce(0, t_stat, t_cols)
    part_with(t_y, t_leave, 0, t_y_edges)
    phase("conv_s")
    settle(got_b_s)
    convolve(s_in, (w_s, b_s), s_y, s_stat, 1)
    phase("mend_s")
    mend(s_y, s_stat, s_owed, 0, 1, s_edges, 1)
    announce(1, s_stat, s_cols)
    part_with(s_y, s_leave, 1, s_y_edges)
    settle(got_small)
    tick()
    phase("conv_e")
    settle(got_b_e)
    convolve(e_in, (w_e, b_e), e_y, e_stat, 0)
    phase("mend_e")
    arrive(fine_base)
    mend(e_y, e_stat, e_owed, 1, 1, e_edges, 0)
    announce(5, e_stat, e_cols)
    tick()
    phase("q_blocks_b")
    q_blocks()
    phase("gather_t")
    norm = gather(0, t_rows, t_cols)
    settle(got_i[1])
    phase("frame_t")
    frame(t_y, t_land, 0, t_y_edges)
    phase("grow_t")
    grow(t_y, t_grown, up_t, activation(norm, 3))
    phase("conv_t2")
    convolve(t_grown, (w_i.at[1], b_i.at[1]), t_y2, t_stat2, 1)
    phase("announce_t2")
    announce(2, t_stat2, 2 * t_cols)
    part_with(t_y2, t_leave2, 2, t_y2_edges)
    tick()
    phase("gather_s")
    norm = gather(1, s_rows, s_cols)
    settle(got_i[0])
    phase("frame_s")
    frame(s_y, s_land, 1, s_y_edges)
    phase("grow_s")
    grow(s_y, s_grown, up_s, activation(norm, 2))
    phase("conv_s2")
    convolve(s_grown, (w_i.at[0], b_i.at[0]), s_y2, s_stat2, 0)
    announce(3, s_stat2, 2 * s_cols)
    tick()
    phase("q_blocks_c")
    q_blocks()
    phase("gather_t2")
    norm = gather(2, 2 * t_rows, 2 * t_cols)
    settle(got_i[2])
    phase("frame_t2")
    frame(t_y2, t_land2, 2, t_y2_edges)
    phase("grow_t2")
    grow(t_y2, t_grown2, up_s, activation(norm, 5))
    phase("conv_t3")
    convolve(t_grown2, (w_i.at[2], b_i.at[2]), t_y3, t_stat3, 1)
    phase("announce_t3")
    announce(4, t_stat3, 4 * t_cols)
    part_with(t_y3, t_leave3, 4, t_y3_edges)
    phase("mend_q")
    mend(q_y, q_stat, q_owed, 1, 0, q_edges, 0)
    announce(6, q_stat, q_cols)
    phase("gather_se")
    s_act = activation(gather(3, 2 * s_rows, 2 * s_cols), 4)
    e_act = activation(gather(5, e_rows, e_cols), 1)
    phase("project")
    class_f[...] = jnp.zeros(class_f.shape, F32)
    class_f[0:classes] = class_w[...].astype(F32)
    class_pad[...] = class_f[...].astype(BF16)
    padded = class_f.shape[0]
    weight = class_pad[...]
    weights = jnp.concatenate([weight] * 2, axis=1)
    across = (((1,), (1,)), ((), ()))

    def project(row, carry):
        lines = jnp.concatenate([e_act(e_y[row]), s_act(s_y2[row])], axis=1)
        coarse[row + 1] = lax.dot_general(weights, lines, across, preferred_element_type=F32)
        return carry

    lax.fori_loop(0, e_rows, project, 0, unroll=4)
    rim_leave[0] = coarse[1].astype(BF16)
    rim_leave[1] = coarse[e_rows].astype(BF16)
    send(coarse_edges)
    coarse[0] = jnp.zeros(coarse.shape[1:], F32)
    coarse[e_rows + 1] = jnp.zeros(coarse.shape[1:], F32)
    up_cols = doubling(e_cols, q_cols, 0)

    phase("gather_t3")
    t_act = activation(gather(4, 4 * t_rows, 4 * t_cols), 6)
    phase("frame_t3")
    frame(t_y3, t_land3, 4, t_y3_edges)
    phase("project_t")

    def project_t(row, carry):
        coarse[row] += lax.dot_general(
            weight, t_act(t_y3[row]), across, preferred_element_type=F32
        )
        return carry

    lax.fori_loop(0, e_rows + 2, project_t, 0, unroll=True)
    phase("wait_coarse")
    arrive(coarse_edges)
    for beyond, row, own, side in ((me == 0, 0, 1, 0), (me == size - 1, e_rows + 1, e_rows, 1)):

        @pl.when(beyond)
        def _():
            coarse[row] = coarse[own]

        @pl.when(jnp.logical_not(beyond))
        def _():
            coarse[row] += rim_land[side].astype(F32)

    phase("widen")
    lines = coarse[...].reshape((e_rows + 2) * padded, e_cols)
    high = lines.astype(BF16)
    low = (lines - high.astype(F32)).astype(BF16)
    lines = jnp.dot(high, up_cols, preferred_element_type=F32) + jnp.dot(
        low, up_cols, preferred_element_type=F32
    )
    wide[...] = lines.reshape(wide.shape)
    phase("gather_q")
    spot = lax.broadcasted_iota(jnp.int32, (padded, classes), 0)
    lane = lax.broadcasted_iota(jnp.int32, (padded, classes), 1)
    bias_col = jnp.sum(jnp.where(spot == lane, bias[...], 0.0), axis=1, keepdims=True)
    q_act = activation(gather(6, q_rows, q_cols), 0)
    phase("finish")
    kind = lax.broadcasted_iota(jnp.int32, (padded, q_cols), 0)

    def finish(row, grown):
        line = lax.dot_general(weight, q_act(q_y[row]), across, preferred_element_type=F32)
        line = line + bias_col + grown
        scores[row] = line
        powers = jnp.where(kind < classes, jnp.exp(line), 0.0)
        log_total = jnp.log(jnp.sum(powers, axis=0, keepdims=True))
        label = labels[pl.ds(row, 1), :]
        picked = jnp.sum(jnp.where(kind == label, line, 0.0), axis=0, keepdims=True)
        usable = label != IGNORED
        return jnp.where(usable, log_total - picked, 0.0), usable.astype(F32)

    def pair(index, carry):
        here = wide[index + 1]
        upper = finish(2 * index, 0.25 * wide[index] + 0.75 * here)
        lower = finish(2 * index + 1, 0.75 * here + 0.25 * wide[index + 2])
        return carry[0] + upper[0] + lower[0], carry[1] + upper[1] + lower[1]

    zero = jnp.zeros((1, q_cols), F32)
    sums = lax.fori_loop(0, e_rows, pair, (zero, zero), unroll=4)
    phase("loss_send")
    for place, line in enumerate(sums):
        loss_slab[place : place + 1] = sum(
            line[:, k * width : (k + 1) * width] for k in range(q_cols // width)
        )

    def loss_copy(source, target, peer):
        return pltpu.make_async_remote_copy(
            src_ref=source,
            dst_ref=target,
            send_sem=loss_send.at[0],
            recv_sem=loss_recv.at[0],
            device_id=peer,
            device_id_type=MESH,
        )

    for peer in reversed(peers):
        loss_copy(loss_slab, loss_slabs.at[flat], peer).start()
    rest = loss_slabs.at[0 : total - 1]
    loss_all = loss_copy(rest, rest, peers[0])
    loss_slabs[flat] = loss_slab[...]
    phase("output")
    for first in range(0, classes, 8):
        lines = jnp.transpose(scores[:, first : first + 8], (1, 0, 2)).astype(BF16)
        out[first : min(first + 8, classes)] = lines[: min(8, classes - first)]
    phase("leave")
    for pairs in (
        t_edges, s_edges, t_y_edges, s_y_edges, t_y2_edges, t_y3_edges, coarse_edges, e_edges, q_edges, coarse_base, fine_base,
    ):
        leave(pairs)
    for number in range(slab.shape[0]):
        slab_all(number).wait_send()
    phase("loss_wait")
    loss_all.wait_recv()
    phase("loss_end")
    ends = jnp.sum(jnp.sum(loss_slabs[...], axis=0), axis=1, keepdims=True)
    loss_out[...] = jnp.broadcast_to(ends[0:1] / jnp.maximum(ends[1:2], 1.0), loss_out.shape)
    loss_all.wait_send()
    phase("")


def make_per_device(shape):
    def per_device(
        feat_quarter,
        feat_eighth,
        feat_sixteenth,
        feat_thirty,
        labels,
        first_weights,
        inner_weights,
        norm_gain,
        norm_shift,
        class_weight,
        class_bias,
    ):
        q, e, s, t = feat_quarter[0], feat_eighth[0], feat_sixteenth[0], feat_thirty[0]
        size = shape["rows"]
        total = size * shape["batch"]
        depth, width = first_weights.shape[3:]
        classes = class_weight.shape[1]
        padded = -(-classes // 8) * 8
        (q_rows, q_cols), (e_rows, e_cols) = q.shape[:2], e.shape[:2]
        (s_rows, s_cols), (t_rows, t_cols) = s.shape[:2], t.shape[:2]

        def framed(rows, cols, channels, kind=BF16):
            return pltpu.VMEM((rows + 2, cols, channels), kind)

        def field(rows, cols):
            return pltpu.VMEM((rows, cols, width), F32)

        def stat(rows):
            return pltpu.VMEM((rows, 8, width), F32)

        def line(cols):
            return pltpu.VMEM((2, cols, width), BF16)

        small = [labels[0], norm_gain, norm_shift, class_weight.T, class_bias[None]]
        scratch = [
            *[pltpu.VMEM(x.shape, x.dtype) for x in small],
            framed(q_rows, q_cols, depth),
            framed(e_rows, e_cols, depth),
            framed(s_rows, s_cols, depth),
            framed(t_rows, t_cols, depth),
            *[pltpu.VMEM((3 * depth, 3 * width), BF16)] * 4,
            pltpu.VMEM((3, 3 * width, 3 * width), BF16),
            *[pltpu.VMEM((4 * depth, 2 * width), BF16)] * 4,
            pltpu.VMEM((3, 4 * width, 2 * width), BF16),
            field(q_rows, q_cols),
            field(e_rows, e_cols),
            framed(s_rows, s_cols, width, F32),
            framed(t_rows, t_cols, width, F32),
            framed(2 * s_rows, 2 * s_cols, width),
            field(2 * s_rows, 2 * s_cols),
            framed(2 * t_rows, 2 * t_cols, width),
            framed(2 * t_rows, 2 * t_cols, width, F32),
            framed(4 * t_rows, 4 * t_cols, width),
            framed(4 * t_rows, 4 * t_cols, width, F32),
            *[
                line(c)
                for c in (t_cols, s_cols, 2 * t_cols, 4 * t_cols, t_cols, s_cols, e_cols, q_cols)
            ]
            * 2,
            *[pltpu.VMEM((2, 2, 2, width), F32)] * 2,
            *[pltpu.VMEM((2, padded, e_cols), BF16)] * 2,
            stat(q_rows),
            stat(e_rows),
            stat(s_rows),
            stat(t_rows),
            stat(2 * s_rows),
            stat(2 * t_rows),
            stat(4 * t_rows),
            pltpu.VMEM((7, 2, width), F32),
            pltpu.VMEM((7, size, 2, width), F32),
            pltpu.VMEM((padded, width), F32),
            pltpu.VMEM((padded, width), BF16),
            pltpu.VMEM((2 * t_cols, t_cols), BF16),
            pltpu.VMEM((2 * s_cols, s_cols), BF16),
            framed(e_rows, padded, e_cols, F32),
            framed(e_rows, padded, q_cols, F32),
            pltpu.VMEM((q_rows, padded, q_cols), F32),
            pltpu.VMEM((2, width), F32),
            pltpu.VMEM((total, 2, width), F32),
            *[pltpu.SemaphoreType.DMA((count,)) for count in (32, 22, 22, 7, 7, 1, 1)],
        ]
        away, held = pl.BlockSpec(memory_space=pl.ANY), pl.BlockSpec(memory_space=pltpu.VMEM)
        operands = (q, e, s, t, small[0], first_weights, inner_weights, *small[1:])
        logits, loss = pl.pallas_call(
            functools.partial(head_kernel, shape),
            out_shape=(
                jax.ShapeDtypeStruct((classes, q_rows, q_cols), BF16),
                jax.ShapeDtypeStruct((8, width), F32),
            ),
            in_specs=[away] * 11,
            out_specs=(held, held),
            scratch_shapes=scratch,
            compiler_params=pltpu.CompilerParams(
                collective_id=0, has_side_effects=True, vmem_limit_bytes=32 << 20
            ),
        )(*[pltpu.with_memory_space_constraint(x, pltpu.HBM) for x in operands])
        return (logits[None], loss[0, 0])

    return per_device


def solution(mesh):
    in_specs = (
        P("batch", "rows", None, None),
        P("batch", "rows", None, None),
        P("batch", "rows", None, None),
        P("batch", "rows", None, None),
        P("batch", "rows", None),
        P(),
        P(),
        P(),
        P(),
        P(),
        P(),
    )
    out_specs = (P("batch", None, "rows", None), P())
    return jax.shard_map(
        make_per_device(dict(mesh.shape)),
        mesh=mesh,
        in_specs=in_specs,
        out_specs=out_specs,
        check_vma=False,
    )
```
